128 devices in a mesh: grp: 8 (over x_hi, y), mem: 16 (over z, x_lo, core).
Axes of the slice: x: 4 (x_hi: 2, x_lo: 2; x = x_hi * 2 + x_lo), y: 4, z: 4, core: 2. Of those that a mesh axis runs over, the one named last changes fastest.
Arguments:
- params: float32 [8, 2048, 2048], P('grp', 'mem'), may hold values from -6 to 6
- estimate: float32 [8, 2048, 2048], P('grp', 'mem'), may hold values from -6 to 6
- mixed_sum: float32 [8, 2048, 2048], P('grp', 'mem'), may hold values from -6 to 6
- activations: bfloat16 [131072, 2048], P(('grp', 'mem')), may hold values from -24 to 24
- out_grads: bfloat16 [131072, 2048], P(('grp', 'mem')), may hold values from -6 to 6
- exponents: int32 [8, 32], P('grp', 'mem'), may hold values from 0 to 3
- edge_weight: float32 [8], replicated, may hold values from 0.1 to 0.45
Outputs:
- new_params: float32 [8, 2048, 2048], P('grp', 'mem')
- new_estimate: float32 [8, 2048, 2048], P('grp', 'mem')
- new_mixed: float32 [8, 2048, 2048], P('grp', 'mem')
The draws below stay inside these ranges and needn't reach their ends.
All inputs are finite; a program needn't handle non-finite values.
Results may differ from the reference program's by a relative error of at most 0.01.
Values may be sent and summed in bfloat16 or wider, within the bound.
No kernel may reach another device: no remote copies, remote signals or barrier semaphores. Data moves between devices by JAX's collectives and lax.ppermute only.
A program may use at most 128 MiB of HBM per device.

```python
import math
import jax
import jax.numpy as jnp
from jax import lax

D = 2048
INNER = 2048
TOK_DEV = 1024
BLOCK = 64
GROUPS = 8
ROWS = 131072
N_MEM = 16


def plant(entries, key, low, top_value):
    spot = [jax.random.randint(jax.random.fold_in(key, axis), (), 0, length) for axis, length in enumerate(entries.shape)]
    longest = entries.shape.index(max(entries.shape))
    neighbour = spot[:longest] + [(spot[longest] + 1) % entries.shape[longest]] + spot[longest + 1:]
    return entries.at[tuple(spot)].set(low).at[tuple(neighbour)].set(top_value)


def strengthened(array, stream_key, source, target, blocks, factor):
    def block_of(dim):
        return (jnp.arange(array.shape[dim]) // (array.shape[dim] // blocks)).reshape((-1,) + (1,) * (array.ndim - 1 - dim))

    first = jax.random.permutation(stream_key, blocks)[block_of(target)]
    second = (block_of(target) + blocks // 2) % blocks
    return jnp.where((block_of(source) == first) | (block_of(source) == second), factor * array, array)


def block_scale(stream_key, shape, cuts, smallest, largest):
    loudness, own = 1.0, jax.random.fold_in(stream_key, 6)
    for dim, shards_of in cuts:
        steps = jnp.exp(jax.random.uniform(jax.random.fold_in(own, dim), (shards_of,), jnp.float32, smallest / len(cuts), largest / len(cuts)))
        loudness = loudness * jnp.repeat(steps, shape[dim] // shards_of).reshape([-1 if axis == dim else 1 for axis in range(len(shape))])
    return loudness


def scatter_about(key, extent, scale, bound, pieces=(), dtype=jnp.bfloat16):
    drawn = jax.random.normal(key, extent, jnp.float32) * scale
    if len(pieces) > 0:
        drawn = block_scale(key, extent, pieces, -0.22, 0.18) * drawn
    return jnp.clip(drawn, min=-bound, max=bound).astype(dtype)


def gaussian_with(own_key, extent, spread, most, pieces, heavy, dtype=jnp.bfloat16):
    entries = spread * jax.random.normal(own_key, extent, jnp.float32)
    if pieces:
        entries = entries * block_scale(own_key, extent, pieces, -0.22, 0.18)
    return jnp.clip(strengthened(entries, jax.random.fold_in(own_key, 3), *heavy), -most, most).astype(dtype)


def setup_inputs(seed: int = 0) -> dict:
    key_list = jax.random.split(jax.random.key(seed), 8)
    params = scatter_about(key_list[0], (GROUPS, D, INNER), 1.0, 6.0, ((0, 8), (1, 16)), jnp.float32)
    estimate = scatter_about(key_list[1], (GROUPS, D, INNER), 1.0, 6.0, ((0, 8), (1, 16)), jnp.float32)
    mixed_sum = scatter_about(key_list[2], (GROUPS, D, INNER), 1.0, 6.0, ((0, 8), (1, 16)), jnp.float32)
    activations = gaussian_with(key_list[3], (ROWS, D), 1.0, 24.0, ((0, 128),), (0, 1, 128, 5.5))
    out_grads = scatter_about(key_list[4], (ROWS, INNER), 1.0, 6.0, ((0, 128),))
    exponents = plant(jax.random.randint(key_list[5], (GROUPS, D // BLOCK), 0, 4), jax.random.fold_in(key_list[5], 1), 0, 3).astype(jnp.int32)
    edge_weight = jnp.clip(jax.random.uniform(key_list[6], (GROUPS,), jnp.float32, 0.1, 0.45), 0.1, 0.45)
    return dict(params=params, estimate=estimate, mixed_sum=mixed_sum, activations=activations, out_grads=out_grads, exponents=exponents, edge_weight=edge_weight)


step_size = 0.5
mixing_rate = 0.4

def reference(params, estimate, mixed_sum, activations, out_grads, exponents, edge_weight):
    groups = params.shape[0]
    group_acts = activations.reshape(groups, N_MEM, TOK_DEV, D)
    group_outs = out_grads.reshape(groups, N_MEM, TOK_DEV, INNER)

    def group_gradient(blocks):

        def accumulate(running, member):
            partial_value = lax.dot_general(member[0], member[1], (((0,), (0,)), ((), ())), preferred_element_type=jnp.float32)
            rounded = lax.optimization_barrier(partial_value.astype(jnp.bfloat16))
            return (running + rounded.astype(jnp.float32), None)
        running, _ = lax.scan(accumulate, jnp.zeros((D, INNER), jnp.float32), blocks)
        return running
    gradient = lax.map(group_gradient, (group_acts, group_outs))
    factor = step_size / math.sqrt(N_MEM * TOK_DEV)
    stepped = params - factor * gradient
    change = stepped - estimate
    scales = jnp.exp2(exponents.astype(jnp.float32))[:, :, None, None]
    blocked = change.reshape(groups, D // BLOCK, BLOCK, INNER)
    levels = lax.optimization_barrier(jnp.clip(blocked / scales, -1.0, 1.0).astype(jnp.bfloat16))
    compressed = (levels.astype(jnp.float32) * scales).astype(jnp.bfloat16).reshape(groups, D, INNER)
    own_piece = compressed.astype(jnp.float32)
    new_estimate = estimate + own_piece
    left_piece = jnp.roll(compressed, 1, axis=0).astype(jnp.float32)
    right_piece = jnp.roll(compressed, -1, axis=0).astype(jnp.float32)
    weight_right = edge_weight
    weight_left = jnp.roll(edge_weight, 1)
    weight_self = 1.0 - weight_left - weight_right
    new_mixed = mixed_sum + weight_self[:, None, None] * own_piece
    new_mixed = new_mixed + weight_left[:, None, None] * left_piece
    new_mixed = new_mixed + weight_right[:, None, None] * right_piece
    new_params = stepped + mixing_rate * (new_mixed - new_estimate)
    return (new_params, new_estimate, new_mixed)
```

```python
import functools
import math

import jax
import jax.numpy as jnp
from jax import lax
from jax.experimental import pallas as pl
from jax.experimental.pallas import tpu as pltpu
from jax.sharding import PartitionSpec as P


step_size = 0.5
mixing_rate = 0.4


f32 = jnp.float32
bf16 = jnp.bfloat16
ANY = pl.BlockSpec(memory_space=pl.ANY)
BLOCK = 128
CHUNKS = 4


def member(z, x, c):
    return z * 4 + x * 2 + c


def moved(value, to):
    pairs = []
    for z in range(4):
        for x in range(2):
            for c in range(2):
                pairs.append((member(z, x, c), member(*to(z, x, c))))
    return lax.ppermute(value, "mem", pairs)


def to_partner(value):
    return moved(value, lambda z, x, c: (z, x, 1 - c))


def to_side(value):
    return moved(value, lambda z, x, c: (z, 1 - x, c))


def up(value):
    return moved(value, lambda z, x, c: ((z + 1) % 4, x, c))


def down(value):
    return moved(value, lambda z, x, c: ((z + 3) % 4, x, c))


def around(value, steps):
    return lax.ppermute(value, "grp", [(g, (g + steps) % 8) for g in range(8)])


FIRST = (
    ((2, 0), (2, 1), 0),
    ((2, 1), (0, 1), 1),
    ((1, 1), (3, 1), 1),
)
SECOND = (
    ((1, 0), (1, 1), 0),
    ((3, 0), (3, 1), 0),
    ((0, 0), (0, 1), 0),
    ((2, 0), (0, 0), 1),
    ((1, 0), (3, 0), 1),
)


def products(activations, out_grads, tasks, own, outs, arrived=None, after=()):
    depth, _ = activations.shape
    width = out_grads.shape[1]
    half = width // 2
    count = len(tasks)
    piece = half // CHUNKS
    operands = [activations, out_grads]
    if arrived is not None:
        operands.append(arrived)
    operands += list(after)
    if outs is None:
        shapes = [jax.ShapeDtypeStruct((count * 2 * BLOCK, half), bf16)]
    else:
        shapes = [
            jax.ShapeDtypeStruct((2 * BLOCK if part is None else BLOCK, half), bf16)
            for _, part in outs
        ]
    copies_out = count if outs is None else len(outs)

    def body(*refs):
        a_ref, g_ref = refs[0], refs[1]
        out_refs = refs[len(operands) : len(operands) + len(shapes)]
        lhs, rhs, extra, value, lhs_sem, rhs_sem, extra_sem, out_sem = refs[
            len(operands) + len(shapes) :
        ]
        index = lax.axis_index("mem")
        z, x, c = index // 4, lax.rem(index // 2, 2), lax.rem(index, 2)
        core = c if own else 1 - c

        def left(t, p):
            dz, dx = tasks[t][p]
            block = lax.rem(z + dz, 4) * 4 + lax.rem(x + dx, 2) * 2 + core
            return pltpu.make_async_copy(
                a_ref.at[:, pl.ds(pl.multiple_of(block * BLOCK, BLOCK), BLOCK)],
                lhs.at[t, :, pl.ds(p * BLOCK, BLOCK)],
                lhs_sem.at[t, p],
            )

        def right(h, j):
            cut = pl.ds(h * half + j * piece, piece)
            return pltpu.make_async_copy(g_ref.at[:, cut], rhs.at[:, cut], rhs_sem.at[h, j])

        def added(t):
            return pltpu.make_async_copy(
                refs[2].at[pl.ds(t * 2 * BLOCK, 2 * BLOCK)], extra.at[t], extra_sem.at[t]
            )

        def given(k):
            if outs is None:
                return pltpu.make_async_copy(
                    value.at[k], out_refs[0].at[pl.ds(k * 2 * BLOCK, 2 * BLOCK)], out_sem.at[k]
                )
            task, part = outs[k]
            source = value.at[task]
            if part is not None:
                source = value.at[task, pl.ds(part * BLOCK, BLOCK)]
            return pltpu.make_async_copy(source, out_refs[k], out_sem.at[k])

        left(0, 0).start()
        left(0, 1).start()
        for j in range(CHUNKS):
            right(0, j).start()
        if arrived is not None:
            added(0).start()
        for t in range(1, count):
            left(t, 0).start()
            left(t, 1).start()
            if arrived is not None:
                added(t).start()
            if tasks[t][2] != tasks[t - 1][2]:
                for j in range(CHUNKS):
                    right(1, j).start()
        for t in range(count):
            h = tasks[t][2]
            fresh = t == 0 or tasks[t - 1][2] != h
            left(t, 0).wait()
            left(t, 1).wait()
            if arrived is not None:
                added(t).wait()
            for j in range(CHUNKS):
                if fresh:
                    right(h, j).wait()
                cut = pl.ds(j * piece, piece)
                total = lax.dot_general(
                    lhs[t],
                    rhs[:, pl.ds(h * half + j * piece, piece)],
                    (((0,), (0,)), ((), ())),
                    preferred_element_type=f32,
                )
                if arrived is not None:
                    total = total + extra[t, :, cut].astype(f32)
                value[t, :, cut] = total.astype(bf16)
            for k in range(copies_out):
                if (k if outs is None else outs[k][0]) == t:
                    given(k).start()
        for k in range(copies_out):
            given(k).wait()

    return pl.pallas_call(
        body,
        in_specs=[ANY] * len(operands),
        out_specs=[ANY] * len(shapes),
        out_shape=shapes,
        scratch_shapes=[
            pltpu.VMEM((count, depth, 2 * BLOCK), bf16),
            pltpu.VMEM((depth, width), bf16),
            pltpu.VMEM((count, 2 * BLOCK, half), bf16),
            pltpu.VMEM((count, 2 * BLOCK, half), bf16),
            pltpu.SemaphoreType.DMA((count, 2)),
            pltpu.SemaphoreType.DMA((2, CHUNKS)),
            pltpu.SemaphoreType.DMA((count,)),
            pltpu.SemaphoreType.DMA((copies_out,)),
        ],
        compiler_params=pltpu.CompilerParams(vmem_limit_bytes=60 << 20),
        cost_estimate=pl.CostEstimate(
            flops=2 * count * 2 * BLOCK * half * depth,
            bytes_accessed=2 * (depth * width + count * 2 * BLOCK * (half + depth)),
            transcendentals=0,
        ),
    )(*operands)


def rows_of(value, start=0, size=None):
    return (value, start, value.shape[0] if size is None else size)


def added(sums, into=None):
    operands, in_specs = [], []
    for terms in sums:
        for value, start, size in terms:
            operands.append(value)
            in_specs.append(
                pl.BlockSpec((size, value.shape[1]), functools.partial(lambda s, i: (s, 0), start // size))
            )
    if into is None:
        shapes = [jax.ShapeDtypeStruct((t[0][2], t[0][0].shape[1]), bf16) for t in sums]
        out_specs = [pl.BlockSpec(s.shape, lambda i: (0, 0)) for s in shapes]
        aliases = {}
    else:
        shapes = [jax.ShapeDtypeStruct(into.shape, bf16)]
        out_specs = [in_specs[0]]
        aliases = {0: 0}

    def body(*refs):
        at = 0
        for terms, out in zip(sums, refs[len(operands) :]):
            total = refs[at][...].astype(f32)
            for k in range(1, len(terms)):
                total = total + refs[at + k][...].astype(f32)
            out[...] = total.astype(bf16)
            at += len(terms)

    return pl.pallas_call(
        body,
        grid=(1,),
        in_specs=in_specs,
        out_specs=out_specs,
        out_shape=shapes,
        input_output_aliases=aliases,
        compiler_params=pltpu.CompilerParams(vmem_limit_bytes=16 << 20),
        cost_estimate=pl.CostEstimate(flops=1 << 20, bytes_accessed=1 << 20, transcendentals=0),
    )(*operands)


STEPS = 4


def compress(side, factor, params, estimate, mixed_sum, exponents, edge_weight, terms, held):
    rows, width = params.shape[1:]
    half = width // 2
    size = rows // STEPS
    span = rows // exponents.shape[1]
    big = pl.BlockSpec((1, size, half), lambda i: (0, i, side))
    small = pl.BlockSpec((size, half), lambda i: (i, 0))
    smem = pl.BlockSpec(memory_space=pltpu.SMEM)
    operands = [exponents, edge_weight, params, estimate, mixed_sum]
    in_specs = [smem, smem, big, big, big]
    for value, start in terms:
        operands.append(value)
        in_specs.append(pl.BlockSpec((size, half), lambda i, s=start // size: (s + i, 0)))
    aliases = {}
    if held is not None:
        aliases = {len(operands): 3}
        operands.append(held)
        in_specs.append(ANY)

    def body(*refs):
        e_ref, w_ref, p_ref, s_ref, m_ref = refs[:5]
        comp_ref, base_ref, rest_ref, est_ref = refs[len(operands) :]
        exponent = e_ref[0, pl.program_id(0) * size // span]
        scale = jnp.left_shift(jnp.int32(1), exponent).astype(f32)
        inverse = jnp.left_shift(jnp.int32(1), 24 - exponent).astype(f32) * (2.0**-24)
        group = lax.axis_index("grp")
        right, left = w_ref[group], w_ref[lax.rem(group + 7, 8)]
        own_weight = 1.0 - left - right
        gradient = refs[5][...].astype(f32)
        for k in range(1, len(terms)):
            gradient = gradient + refs[5 + k][...].astype(f32)
        old = s_ref[0]
        stepped = p_ref[0] - factor * gradient
        levels = jnp.clip((stepped - old) * inverse, -1.0, 1.0).astype(bf16)
        own = levels.astype(f32) * scale
        new = old + own
        comp_ref[...] = own.astype(bf16)
        base_ref[...] = m_ref[0] + own_weight * own
        rest_ref[...] = stepped - mixing_rate * new
        est_ref[0] = new

    return pl.pallas_call(
        body,
        grid=(STEPS,),
        in_specs=in_specs,
        out_specs=[small, small, small, big],
        out_shape=[
            jax.ShapeDtypeStruct((rows, half), bf16),
            jax.ShapeDtypeStruct((rows, half), f32),
            jax.ShapeDtypeStruct((rows, half), f32),
            jax.ShapeDtypeStruct(params.shape, f32),
        ],
        input_output_aliases=aliases,
        compiler_params=pltpu.CompilerParams(vmem_limit_bytes=16 << 20),
        cost_estimate=pl.CostEstimate(flops=2 << 20, bytes_accessed=4 << 20, transcendentals=0),
    )(*operands)


def finish(side, edge_weight, base, rest, from_left, from_right, held, shape):
    rows, width = shape[1:]
    half = width // 2
    size = rows // STEPS
    big = pl.BlockSpec((1, size, half), lambda i: (0, i, side))
    small = pl.BlockSpec((size, half), lambda i: (i, 0))
    operands = [edge_weight, base, rest, from_left, from_right]
    in_specs = [pl.BlockSpec(memory_space=pltpu.SMEM), small, small, small, small]
    aliases = {}
    if held is not None:
        aliases = {len(operands): 0, len(operands) + 1: 1}
        operands += list(held)
        in_specs += [ANY, ANY]

    def body(*refs):
        w_ref, base_ref, rest_ref, left_ref, right_ref = refs[:5]
        new_params, new_mixed = refs[len(operands) :]
        group = lax.axis_index("grp")
        right, left = w_ref[group], w_ref[lax.rem(group + 7, 8)]
        mixed = base_ref[...] + left * left_ref[...].astype(f32)
        mixed = mixed + right * right_ref[...].astype(f32)
        new_mixed[0] = mixed
        new_params[0] = rest_ref[...] + mixing_rate * mixed

    return pl.pallas_call(
        body,
        grid=(STEPS,),
        in_specs=in_specs,
        out_specs=[big, big],
        out_shape=[jax.ShapeDtypeStruct(shape, f32)] * 2,
        input_output_aliases=aliases,
        compiler_params=pltpu.CompilerParams(vmem_limit_bytes=16 << 20),
        cost_estimate=pl.CostEstimate(flops=1 << 20, bytes_accessed=3 << 20, transcendentals=0),
    )(*operands)


def on_device(params, estimate, mixed_sum, activations, out_grads, exponents, edge_weight):
    factor = step_size / math.sqrt(lax.axis_size("mem") * activations.shape[0])
    half_block = BLOCK // 2
    terms_1 = products(activations, out_grads, FIRST, False, None)[0]
    swapped_1 = to_partner(terms_1)
    terms_2 = products(activations, out_grads, SECOND, False, None, after=[terms_1])[0]
    swapped_2 = to_partner(terms_2)
    a_up, a_down, b_far, b_own, b_near = products(
        activations, out_grads, FIRST, True,
        [(0, 0), (0, 1), (1, 0), (1, 1), (2, None)], swapped_1, [terms_2],
    )
    got_far = to_side(b_far)
    got_up, got_down = up(a_up), down(a_down)
    got_near, got_own = to_side(b_near), to_side(b_own)
    near_up, near_down, own, keep_1, keep_2 = products(
        activations, out_grads, SECOND, True,
        [(0, None), (1, None), (2, None), (3, None), (4, None)], swapped_2, [a_up],
    )
    far_low, far_high = added(
        [
            [rows_of(keep_1, 0, half_block), rows_of(got_far, 0, half_block)],
            [rows_of(keep_1, half_block, half_block), rows_of(got_far, half_block, half_block)],
        ],
    )
    far_low, far_high = up(far_low), down(far_high)
    send_up = added([[rows_of(near_up, 0, BLOCK), rows_of(got_up)]], near_up)[0]
    send_down = added([[rows_of(near_down, BLOCK, BLOCK), rows_of(got_down)]], near_down)[0]
    from_below, from_above = up(send_up), down(send_down)
    v_up, v_down = added(
        [
            [rows_of(keep_2, 0, BLOCK), rows_of(got_near, 0, BLOCK)],
            [rows_of(keep_2, BLOCK, BLOCK), rows_of(got_near, BLOCK, BLOCK)],
        ],
    )
    v_up = added([[rows_of(v_up, 0, half_block), rows_of(far_low)]], v_up)[0]
    v_down = added([[rows_of(v_down, half_block, half_block), rows_of(far_high)]], v_down)[0]
    b_below, b_above = up(v_up), down(v_down)
    side_sum = added(
        [[rows_of(own, BLOCK, BLOCK), rows_of(from_below, BLOCK, BLOCK), rows_of(from_above, BLOCK, BLOCK)]],
    )[0]
    got_side = to_side(side_sum)
    own_parts = (params, estimate, mixed_sum, exponents, edge_weight)
    comp_b, base_b, rest_b, held = compress(
        1, factor, *own_parts, [(keep_1, BLOCK), (got_own, 0), (b_below, 0), (b_above, 0)], None
    )
    left_b, right_b = around(comp_b, 1), around(comp_b, -1)
    comp_a, base_a, rest_a, new_estimate = compress(
        0, factor, *own_parts, [(own, 0), (from_below, 0), (from_above, 0), (got_side, 0)], held
    )
    left_a, right_a = around(comp_a, 1), around(comp_a, -1)
    outs = finish(1, edge_weight, base_b, rest_b, left_b, right_b, None, params.shape)
    new_params, new_mixed = finish(0, edge_weight, base_a, rest_a, left_a, right_a, outs, params.shape)
    return (new_params, new_estimate, new_mixed)


def solution(mesh):
    in_specs = (
        P("grp", "mem", None),
        P("grp", "mem", None),
        P("grp", "mem", None),
        P(("grp", "mem"), None),
        P(("grp", "mem"), None),
        P("grp", "mem"),
        P(),
    )
    out_specs = (P("grp", "mem", None), P("grp", "mem", None), P("grp", "mem", None))
    return jax.shard_map(
        on_device, mesh=mesh, in_specs=in_specs, out_specs=out_specs, check_vma=False
    )
```

```python
import functools
import math

import jax
import jax.numpy as jnp
from jax import lax
from jax.experimental import pallas as pl
from jax.experimental.pallas import tpu as pltpu
from jax.sharding import PartitionSpec as P


step_size = 0.5
mixing_rate = 0.4


f32 = jnp.float32
bf16 = jnp.bfloat16
ANY = pl.BlockSpec(memory_space=pl.ANY)
BLOCK = 128
CHUNKS = 2


def member(z, x, c):
    return z * 4 + x * 2 + c


def moved(value, to):
    pairs = []
    for z in range(4):
        for x in range(2):
            for c in range(2):
                pairs.append((member(z, x, c), member(*to(z, x, c))))
    return lax.ppermute(value, "mem", pairs)


def to_partner(value):
    return moved(value, lambda z, x, c: (z, x, 1 - c))


def to_side(value):
    return moved(value, lambda z, x, c: (z, 1 - x, c))


def up(value):
    return moved(value, lambda z, x, c: ((z + 1) % 4, x, c))


def down(value):
    return moved(value, lambda z, x, c: ((z + 3) % 4, x, c))


def around(value, steps):
    return lax.ppermute(value, "grp", [(g, (g + steps) % 8) for g in range(8)])


SENT_A = (((2, 0), (1, 1)), ((2, 1), (3, 0)))
KEPT_A = (((1, 0), (3, 1)), ((0, 0), (0, 1)))
ALL_B = (((1, 1), (3, 1)), ((2, 1), (0, 1)), ((2, 0), (0, 0)), ((1, 0), (3, 0)))
GROUP = 4


def products(activations, out_grads, side, tasks, after=()):
    depth, _ = activations.shape
    half = out_grads.shape[1] // 2
    piece = half // CHUNKS
    work = [(o, t) for t in range(len(tasks)) for o in (0, 1)]
    count = len(work)
    operands = [activations, out_grads, *after]
    shape = jax.ShapeDtypeStruct((len(tasks) * 2 * BLOCK, half), bf16)

    def body(*refs):
        a_ref, g_ref = refs[:2]
        out_refs = refs[len(operands) : len(operands) + 2]
        lhs, rhs, value, lhs_sem, rhs_sem, out_sem = refs[len(operands) + 2 :]
        index = lax.axis_index("mem")
        z, x, c = index // 4, lax.rem(index // 2, 2), lax.rem(index, 2)

        def left(k, p):
            own, t = work[k]
            dz, dx = tasks[t][p]
            block = lax.rem(z + dz, 4) * 4 + lax.rem(x + dx, 2) * 2 + (c if own else 1 - c)
            return pltpu.make_async_copy(
                a_ref.at[:, pl.ds(pl.multiple_of(block * BLOCK, BLOCK), BLOCK)],
                lhs.at[k // GROUP, :, pl.ds(((k % GROUP) * 2 + p) * BLOCK, BLOCK)],
                lhs_sem.at[k, p],
            )

        def right(j):
            return pltpu.make_async_copy(
                g_ref.at[:, pl.ds(side * half + j * piece, piece)],
                rhs.at[:, pl.ds(j * piece, piece)],
                rhs_sem.at[j],
            )

        def given(k, j):
            own, t = work[k]
            cut = pl.ds(j * piece, piece)
            return pltpu.make_async_copy(
                value.at[k, :, cut],
                out_refs[own].at[pl.ds(t * 2 * BLOCK, 2 * BLOCK), cut],
                out_sem.at[k, j],
            )

        for k in range(count):
            left(k, 0).start()
            left(k, 1).start()
            if k == GROUP - 1:
                for j in range(CHUNKS):
                    right(j).start()
        for first in range(0, count, GROUP):
            for k in range(first, first + GROUP):
                left(k, 0).wait()
                left(k, 1).wait()
            for j in range(CHUNKS):
                if first == 0:
                    right(j).wait()
                cut = pl.ds(j * piece, piece)
                total = lax.dot_general(
                    lhs[first // GROUP],
                    rhs[:, cut],
                    (((0,), (0,)), ((), ())),
                    preferred_element_type=f32,
                ).astype(bf16)
                for k in range(first, first + GROUP):
                    at = (k - first) * 2 * BLOCK
                    value[k, :, cut] = total[at : at + 2 * BLOCK]
                    given(k, j).start()
        for k in range(count):
            for j in range(CHUNKS):
                given(k, j).wait()

    return pl.pallas_call(
        body,
        in_specs=[ANY] * len(operands),
        out_specs=[ANY] * 2,
        out_shape=[shape] * 2,
        scratch_shapes=[
            pltpu.VMEM((count // GROUP, depth, GROUP * 2 * BLOCK), bf16),
            pltpu.VMEM((depth, half), bf16),
            pltpu.VMEM((count, 2 * BLOCK, half), bf16),
            pltpu.SemaphoreType.DMA((count, 2)),
            pltpu.SemaphoreType.DMA((CHUNKS,)),
            pltpu.SemaphoreType.DMA((count, CHUNKS)),
        ],
        compiler_params=pltpu.CompilerParams(vmem_limit_bytes=50 << 20),
        cost_estimate=pl.CostEstimate(
            flops=2 * count * 2 * BLOCK * half * depth,
            bytes_accessed=2 * (depth * half + count * 2 * BLOCK * (half + depth)),
            transcendentals=0,
        ),
    )(*operands)


def added(outs, steps=1):
    operands, in_specs = [], []
    width = outs[0][1][0][0].shape[1]
    piece = width // steps
    for _, terms in outs:
        for value, start, size, _ in terms:
            operands.append(value)
            in_specs.append(
                pl.BlockSpec((size, piece), functools.partial(lambda s, i: (s, i), start // size))
            )

    def body(*refs):
        at = 0
        for (rows, terms), out in zip(outs, refs[len(operands) :]):
            edges = sorted({0, rows} | {t[3] for t in terms} | {t[3] + t[2] for t in terms})
            for low, high in zip(edges, edges[1:]):
                total = None
                for k, (_, _, size, place) in enumerate(terms):
                    if place <= low and high <= place + size:
                        value = refs[at + k][low - place : high - place, :].astype(f32)
                        total = value if total is None else total + value
                out[low:high, :] = total.astype(bf16)
            at += len(terms)

    return pl.pallas_call(
        body,
        grid=(steps,),
        in_specs=in_specs,
        out_specs=[pl.BlockSpec((rows, piece), lambda i: (0, i)) for rows, _ in outs],
        out_shape=[jax.ShapeDtypeStruct((rows, width), bf16) for rows, _ in outs],
        compiler_params=pltpu.CompilerParams(vmem_limit_bytes=24 << 20),
        cost_estimate=pl.CostEstimate(flops=1 << 20, bytes_accessed=1 << 20, transcendentals=0),
    )(*operands)


def kernel(body, operands, in_specs, out_specs, out_shape, aliases, steps=1):
    return pl.pallas_call(
        body,
        grid=(steps,),
        in_specs=in_specs,
        out_specs=out_specs,
        out_shape=out_shape,
        input_output_aliases=aliases,
        compiler_params=pltpu.CompilerParams(vmem_limit_bytes=16 << 20),
        cost_estimate=pl.CostEstimate(flops=2 << 20, bytes_accessed=3 << 20, transcendentals=0),
    )(*operands)


SMEM = pl.BlockSpec(memory_space=pltpu.SMEM)


def compress(side, factor, params, estimate, exponents, terms):
    rows, width = params.shape[1:]
    half = width // 2
    span = rows // exponents.shape[1]
    big = pl.BlockSpec((1, rows, half), lambda i: (0, 0, side))
    flat = pl.BlockSpec((rows, half), lambda i: (0, 0))
    operands = [exponents, params, estimate]
    in_specs = [SMEM, big, big]
    for value, start in terms:
        operands.append(value)
        in_specs.append(pl.BlockSpec((rows, half), lambda i, s=start // rows: (s, 0)))

    def body(*refs):
        e_ref, p_ref, s_ref = refs[:3]
        comp_ref, stepped_ref = refs[len(operands) :]
        for part in range(rows // span):
            exponent = e_ref[0, part]
            scale = jnp.left_shift(jnp.int32(1), exponent).astype(f32)
            inverse = jnp.left_shift(jnp.int32(1), 24 - exponent).astype(f32) * (2.0**-24)
            cut = slice(part * span, (part + 1) * span)
            gradient = refs[3][cut, :].astype(f32)
            for k in range(1, len(terms)):
                gradient = gradient + refs[3 + k][cut, :].astype(f32)
            stepped = p_ref[0, cut, :] - factor * gradient
            change = stepped - s_ref[0, cut, :]
            levels = jnp.clip(change * inverse, -1.0, 1.0).astype(bf16)
            comp_ref[cut, :] = (levels.astype(f32) * scale).astype(bf16)
            stepped_ref[cut, :] = stepped

    shapes = [jax.ShapeDtypeStruct((rows, half), bf16), jax.ShapeDtypeStruct((rows, half), f32)]
    return kernel(body, operands, in_specs, [flat, flat], shapes, {})


def own_part(side, estimate, mixed_sum, edge_weight, compressed, stepped, held, after):
    rows, width = estimate.shape[1:]
    half = width // 2
    big = pl.BlockSpec((1, rows, half), lambda i: (0, 0, side))
    flat = pl.BlockSpec((rows, half), lambda i: (0, 0))
    operands = [edge_weight, estimate, mixed_sum, compressed, stepped]
    in_specs = [SMEM, big, big, flat, flat]
    aliases = {}
    if held is not None:
        aliases = {len(operands): 2}
        operands.append(held)
        in_specs.append(ANY)
    operands += after
    in_specs += [ANY] * len(after)

    def body(*refs):
        w_ref, s_ref, m_ref, c_ref, p_ref = refs[:5]
        base_ref, rest_ref, est_ref = refs[len(operands) :]
        group = lax.axis_index("grp")
        right, left = w_ref[group], w_ref[lax.rem(group + 7, 8)]
        own = c_ref[...].astype(f32)
        new = s_ref[0] + own
        base_ref[...] = m_ref[0] + (1.0 - left - right) * own
        rest_ref[...] = p_ref[...] - mixing_rate * new
        est_ref[0] = new

    shapes = [jax.ShapeDtypeStruct((rows, half), f32)] * 2
    shapes.append(jax.ShapeDtypeStruct(estimate.shape, f32))
    return kernel(body, operands, in_specs, [flat, flat, big], shapes, aliases)


def finish(side, edge_weight, base, rest, from_left, from_right, held, shape):
    rows, width = shape[1:]
    half = width // 2
    piece = half // 2
    big = pl.BlockSpec((1, rows, piece), lambda i: (0, 0, side * 2 + i))
    flat = pl.BlockSpec((rows, piece), lambda i: (0, i))
    operands = [edge_weight, base, rest, from_left, from_right]
    in_specs = [SMEM, flat, flat, flat, flat]
    aliases = {}
    if held is not None:
        aliases = {len(operands): 0, len(operands) + 1: 1}
        operands += list(held)
        in_specs += [ANY, ANY]

    def body(*refs):
        w_ref, base_ref, rest_ref, left_ref, right_ref = refs[:5]
        new_params, new_mixed = refs[len(operands) :]
        group = lax.axis_index("grp")
        right, left = w_ref[group], w_ref[lax.rem(group + 7, 8)]
        mixed = base_ref[...] + left * left_ref[...].astype(f32)
        mixed = mixed + right * right_ref[...].astype(f32)
        new_mixed[0] = mixed
        new_params[0] = rest_ref[...] + mixing_rate * mixed

    shapes = [jax.ShapeDtypeStruct(shape, f32)] * 2
    return kernel(body, operands, in_specs, [big, big], shapes, aliases, 2)


def on_device(params, estimate, mixed_sum, activations, out_grads, exponents, edge_weight):
    factor = step_size / math.sqrt(lax.axis_size("mem") * activations.shape[0])
    low = BLOCK // 2
    theirs_1, mine_1 = products(activations, out_grads, 0, SENT_A)
    other_1 = to_partner(theirs_1)
    theirs_2, mine_2 = products(activations, out_grads, 1, ALL_B, [theirs_1])
    other_2 = to_partner(theirs_2)

    def pair(mine, other, start, size, *more):
        return (size, [(mine, start, size, 0), (other, start, size, 0), *more])

    pair_1 = functools.partial(pair, mine_1, other_1)
    pair_2 = functools.partial(pair, mine_2, other_2)
    a_up, a_down = added([pair_1(0, 256), pair_1(256, 256)])
    got_up, got_down = up(a_up), down(a_down)
    b_near, b_far, b_own = added([pair_2(0, 256), pair_2(256, 128), pair_2(384, 128)])
    got_far = to_side(b_far)
    got_near, got_own = to_side(b_near), to_side(b_own)
    theirs_3, mine_3 = products(activations, out_grads, 0, KEPT_A, [a_up, b_far])
    other_3 = to_partner(theirs_3)
    pair_3 = functools.partial(pair, mine_3, other_3)
    far_low, far_high = added(
        [pair_2(512, low, (got_far, 0, low, 0)), pair_2(512 + low, low, (got_far, low, low, 0))],
    )
    far_low, far_high = up(far_low), down(far_high)
    send_up, send_down = added(
        [pair_3(0, BLOCK, (got_up, 0, BLOCK, 0)), pair_3(BLOCK, BLOCK, (got_down, 0, BLOCK, 0))],
    )
    from_below, from_above = up(send_up), down(send_down)
    v_up, v_down = added(
        [
            pair_2(768, BLOCK, (got_near, 0, BLOCK, 0), (far_low, 0, low, 0)),
            pair_2(896, BLOCK, (got_near, BLOCK, BLOCK, 0), (far_high, 0, low, low)),
        ],
    )
    b_below, b_above = up(v_up), down(v_down)
    side_sum = added([pair_3(384, BLOCK, (got_up, BLOCK, BLOCK, 0), (from_above, 0, BLOCK, 0))])[0]
    got_side = to_side(side_sum)
    terms_b = [(mine_2, 640), (other_2, 640), (got_own, 0), (b_below, 0), (b_above, 0)]
    terms_a = [(mine_3, 256), (other_3, 256), (got_down, BLOCK), (from_below, 0), (got_side, 0)]
    comp_b, stepped_b = compress(1, factor, params, estimate, exponents, terms_b)
    left_b, right_b = around(comp_b, 1), around(comp_b, -1)
    comp_a, stepped_a = compress(0, factor, params, estimate, exponents, terms_a)
    left_a, right_a = around(comp_a, 1), around(comp_a, -1)
    own = (estimate, mixed_sum, edge_weight)
    base_b, rest_b, held = own_part(1, *own, comp_b, stepped_b, None, [comp_a])
    base_a, rest_a, new_estimate = own_part(0, *own, comp_a, stepped_a, held, [])
    outs = finish(1, edge_weight, base_b, rest_b, left_b, right_b, None, params.shape)
    new_params, new_mixed = finish(
        0, edge_weight, base_a, rest_a, left_a, right_a, outs, params.shape
    )
    return (new_params, new_estimate, new_mixed)


def solution(mesh):
    in_specs = (
        P("grp", "mem", None),
        P("grp", "mem", None),
        P("grp", "mem", None),
        P(("grp", "mem"), None),
        P(("grp", "mem"), None),
        P("grp", "mem"),
        P(),
    )
    out_specs = (P("grp", "mem", None), P("grp", "mem", None), P("grp", "mem", None))
    return jax.shard_map(
        on_device, mesh=mesh, in_specs=in_specs, out_specs=out_specs, check_vma=False
    )
```

```python
import functools
import math

import jax
import jax.numpy as jnp
from jax import lax
from jax.experimental import pallas as pl
from jax.experimental.pallas import tpu as pltpu
from jax.sharding import PartitionSpec as P


step_size = 0.5
mixing_rate = 0.4


f32 = jnp.float32
bf16 = jnp.bfloat16
ANY = pl.BlockSpec(memory_space=pl.ANY)
BLOCK = 128
CHUNKS = 2


def member(z, x, c):
    return z * 4 + x * 2 + c


def moved(value, to):
    pairs = []
    for z in range(4):
        for x in range(2):
            for c in range(2):
                pairs.append((member(z, x, c), member(*to(z, x, c))))
    return lax.ppermute(value, "mem", pairs)


def to_partner(value):
    return moved(value, lambda z, x, c: (z, x, 1 - c))


def to_side(value):
    return moved(value, lambda z, x, c: (z, 1 - x, c))


def up(value):
    return moved(value, lambda z, x, c: ((z + 1) % 4, x, c))


def down(value):
    return moved(value, lambda z, x, c: ((z + 3) % 4, x, c))


def around(value, steps):
    return lax.ppermute(value, "grp", [(g, (g + steps) % 8) for g in range(8)])


SENT_A = (((2, 0), (1, 1)), ((2, 1), (3, 0)))
KEPT_A = (((1, 0), (3, 1)), ((0, 0), (0, 1)))
SENT_B = (((1, 1), (3, 1)), ((2, 1), (0, 1)))
KEPT_B = (((2, 0), (0, 0)), ((1, 0), (3, 0)))
GROUP = 4


def products(activations, out_grads, side, tasks, after=()):
    depth, _ = activations.shape
    half = out_grads.shape[1] // 2
    piece = half // CHUNKS
    work = [(o, t) for t in range(len(tasks)) for o in (0, 1)]
    count = len(work)
    operands = [activations, out_grads, *after]
    shape = jax.ShapeDtypeStruct((len(tasks) * 2 * BLOCK, half), bf16)

    def body(*refs):
        a_ref, g_ref = refs[:2]
        out_refs = refs[len(operands) : len(operands) + 2]
        lhs, rhs, value, lhs_sem, rhs_sem, out_sem = refs[len(operands) + 2 :]
        index = lax.axis_index("mem")
        z, x, c = index // 4, lax.rem(index // 2, 2), lax.rem(index, 2)

        def left(k, p):
            own, t = work[k]
            dz, dx = tasks[t][p]
            block = lax.rem(z + dz, 4) * 4 + lax.rem(x + dx, 2) * 2 + (c if own else 1 - c)
            return pltpu.make_async_copy(
                a_ref.at[:, pl.ds(pl.multiple_of(block * BLOCK, BLOCK), BLOCK)],
                lhs.at[k // GROUP, :, pl.ds(((k % GROUP) * 2 + p) * BLOCK, BLOCK)],
                lhs_sem.at[k, p],
            )

        def right(j):
            return pltpu.make_async_copy(
                g_ref.at[:, pl.ds(side * half + j * piece, piece)],
                rhs.at[:, pl.ds(j * piece, piece)],
                rhs_sem.at[j],
            )

        def given(k, j):
            own, t = work[k]
            cut = pl.ds(j * piece, piece)
            return pltpu.make_async_copy(
                value.at[k, :, cut],
                out_refs[own].at[pl.ds(t * 2 * BLOCK, 2 * BLOCK), cut],
                out_sem.at[k, j],
            )

        for k in range(count):
            left(k, 0).start()
            left(k, 1).start()
            if k == GROUP - 1:
                for j in range(CHUNKS):
                    right(j).start()
        for first in range(0, count, GROUP):
            for k in range(first, first + GROUP):
                left(k, 0).wait()
                left(k, 1).wait()
            for j in range(CHUNKS):
                if first == 0:
                    right(j).wait()
                cut = pl.ds(j * piece, piece)
                total = lax.dot_general(
                    lhs[first // GROUP],
                    rhs[:, cut],
                    (((0,), (0,)), ((), ())),
                    preferred_element_type=f32,
                ).astype(bf16)
                for k in range(first, first + GROUP):
                    at = (k - first) * 2 * BLOCK
                    value[k, :, cut] = total[at : at + 2 * BLOCK]
                    given(k, j).start()
        for k in range(count):
            for j in range(CHUNKS):
                given(k, j).wait()

    return pl.pallas_call(
        body,
        in_specs=[ANY] * len(operands),
        out_specs=[ANY] * 2,
        out_shape=[shape] * 2,
        scratch_shapes=[
            pltpu.VMEM((count // GROUP, depth, GROUP * 2 * BLOCK), bf16),
            pltpu.VMEM((depth, half), bf16),
            pltpu.VMEM((count, 2 * BLOCK, half), bf16),
            pltpu.SemaphoreType.DMA((count, 2)),
            pltpu.SemaphoreType.DMA((CHUNKS,)),
            pltpu.SemaphoreType.DMA((count, CHUNKS)),
        ],
        compiler_params=pltpu.CompilerParams(vmem_limit_bytes=50 << 20),
        cost_estimate=pl.CostEstimate(
            flops=2 * count * 2 * BLOCK * half * depth,
            bytes_accessed=2 * (depth * half + count * 2 * BLOCK * (half + depth)),
            transcendentals=0,
        ),
    )(*operands)


def added(outs, steps=1):
    operands, in_specs = [], []
    width = outs[0][1][0][0].shape[1]
    piece = width // steps
    for _, terms in outs:
        for value, start, size, _ in terms:
            operands.append(value)
            in_specs.append(
                pl.BlockSpec((size, piece), functools.partial(lambda s, i: (s, i), start // size))
            )

    def body(*refs):
        at = 0
        for (rows, terms), out in zip(outs, refs[len(operands) :]):
            edges = sorted({0, rows} | {t[3] for t in terms} | {t[3] + t[2] for t in terms})
            for low, high in zip(edges, edges[1:]):
                total = None
                for k, (_, _, size, place) in enumerate(terms):
                    if place <= low and high <= place + size:
                        value = refs[at + k][low - place : high - place, :].astype(f32)
                        total = value if total is None else total + value
                out[low:high, :] = total.astype(bf16)
            at += len(terms)

    return pl.pallas_call(
        body,
        grid=(steps,),
        in_specs=in_specs,
        out_specs=[pl.BlockSpec((rows, piece), lambda i: (0, i)) for rows, _ in outs],
        out_shape=[jax.ShapeDtypeStruct((rows, width), bf16) for rows, _ in outs],
        compiler_params=pltpu.CompilerParams(vmem_limit_bytes=24 << 20),
        cost_estimate=pl.CostEstimate(flops=1 << 20, bytes_accessed=1 << 20, transcendentals=0),
    )(*operands)


def kernel(body, operands, in_specs, out_specs, out_shape, aliases, steps=1):
    return pl.pallas_call(
        body,
        grid=(steps,),
        in_specs=in_specs,
        out_specs=out_specs,
        out_shape=out_shape,
        input_output_aliases=aliases,
        compiler_params=pltpu.CompilerParams(vmem_limit_bytes=16 << 20),
        cost_estimate=pl.CostEstimate(flops=2 << 20, bytes_accessed=3 << 20, transcendentals=0),
    )(*operands)


SMEM = pl.BlockSpec(memory_space=pltpu.SMEM)


def compress(side, factor, params, estimate, exponents, terms):
    rows, width = params.shape[1:]
    half = width // 2
    span = rows // exponents.shape[1]
    big = pl.BlockSpec((1, rows, half), lambda i: (0, 0, side))
    flat = pl.BlockSpec((rows, half), lambda i: (0, 0))
    operands = [exponents, params, estimate]
    in_specs = [SMEM, big, big]
    for value, start in terms:
        operands.append(value)
        in_specs.append(pl.BlockSpec((rows, half), lambda i, s=start // rows: (s, 0)))

    def body(*refs):
        e_ref, p_ref, s_ref = refs[:3]
        comp_ref, stepped_ref = refs[len(operands) :]
        for part in range(rows // span):
            exponent = e_ref[0, part]
            scale = jnp.left_shift(jnp.int32(1), exponent).astype(f32)
            inverse = jnp.left_shift(jnp.int32(1), 24 - exponent).astype(f32) * (2.0**-24)
            cut = slice(part * span, (part + 1) * span)
            gradient = refs[3][cut, :].astype(f32)
            for k in range(1, len(terms)):
                gradient = gradient + refs[3 + k][cut, :].astype(f32)
            stepped = p_ref[0, cut, :] - factor * gradient
            change = stepped - s_ref[0, cut, :]
            levels = jnp.clip(change * inverse, -1.0, 1.0).astype(bf16)
            comp_ref[cut, :] = (levels.astype(f32) * scale).astype(bf16)
            stepped_ref[cut, :] = stepped

    shapes = [jax.ShapeDtypeStruct((rows, half), bf16), jax.ShapeDtypeStruct((rows, half), f32)]
    return kernel(body, operands, in_specs, [flat, flat], shapes, {})


def own_part(side, estimate, mixed_sum, edge_weight, compressed, stepped, held, after):
    rows, width = estimate.shape[1:]
    half = width // 2
    big = pl.BlockSpec((1, rows, half), lambda i: (0, 0, side))
    flat = pl.BlockSpec((rows, half), lambda i: (0, 0))
    operands = [edge_weight, estimate, mixed_sum, compressed, stepped]
    in_specs = [SMEM, big, big, flat, flat]
    aliases = {}
    if held is not None:
        aliases = {len(operands): 2}
        operands.append(held)
        in_specs.append(ANY)
    operands += after
    in_specs += [ANY] * len(after)

    def body(*refs):
        w_ref, s_ref, m_ref, c_ref, p_ref = refs[:5]
        base_ref, rest_ref, est_ref = refs[len(operands) :]
        group = lax.axis_index("grp")
        right, left = w_ref[group], w_ref[lax.rem(group + 7, 8)]
        own = c_ref[...].astype(f32)
        new = s_ref[0] + own
        base_ref[...] = m_ref[0] + (1.0 - left - right) * own
        rest_ref[...] = p_ref[...] - mixing_rate * new
        est_ref[0] = new

    shapes = [jax.ShapeDtypeStruct((rows, half), f32)] * 2
    shapes.append(jax.ShapeDtypeStruct(estimate.shape, f32))
    return kernel(body, operands, in_specs, [flat, flat, big], shapes, aliases)


def finish(side, edge_weight, base, rest, from_left, from_right, held, shape):
    rows, width = shape[1:]
    half = width // 2
    piece = half // 2
    big = pl.BlockSpec((1, rows, piece), lambda i: (0, 0, side * 2 + i))
    flat = pl.BlockSpec((rows, piece), lambda i: (0, i))
    operands = [edge_weight, base, rest, from_left, from_right]
    in_specs = [SMEM, flat, flat, flat, flat]
    aliases = {}
    if held is not None:
        aliases = {len(operands): 0, len(operands) + 1: 1}
        operands += list(held)
        in_specs += [ANY, ANY]

    def body(*refs):
        w_ref, base_ref, rest_ref, left_ref, right_ref = refs[:5]
        new_params, new_mixed = refs[len(operands) :]
        group = lax.axis_index("grp")
        right, left = w_ref[group], w_ref[lax.rem(group + 7, 8)]
        mixed = base_ref[...] + left * left_ref[...].astype(f32)
        mixed = mixed + right * right_ref[...].astype(f32)
        new_mixed[0] = mixed
        new_params[0] = rest_ref[...] + mixing_rate * mixed

    shapes = [jax.ShapeDtypeStruct(shape, f32)] * 2
    return kernel(body, operands, in_specs, [big, big], shapes, aliases, 2)


def on_device(params, estimate, mixed_sum, activations, out_grads, exponents, edge_weight):
    factor = step_size / math.sqrt(lax.axis_size("mem") * activations.shape[0])
    low = BLOCK // 2
    theirs_1, mine_1 = products(activations, out_grads, 0, SENT_A)
    other_1 = to_partner(theirs_1)
    theirs_2, mine_2 = products(activations, out_grads, 1, SENT_B, [theirs_1])
    other_2 = to_partner(theirs_2)

    def pair(mine, other, start, size, *more):
        return (size, [(mine, start, size, 0), (other, start, size, 0), *more])

    pair_1 = functools.partial(pair, mine_1, other_1)
    pair_2 = functools.partial(pair, mine_2, other_2)
    a_up, a_down = added([pair_1(0, 256), pair_1(256, 256)])
    got_up, got_down = up(a_up), down(a_down)
    b_near, b_far, b_own = added([pair_2(0, 256), pair_2(256, 128), pair_2(384, 128)])
    got_far = to_side(b_far)
    got_near, got_own = to_side(b_near), to_side(b_own)
    theirs_3, mine_3 = products(activations, out_grads, 1, KEPT_B, [a_up, b_far])
    other_3 = to_partner(theirs_3)
    theirs_4, mine_4 = products(activations, out_grads, 0, KEPT_A, [theirs_3])
    other_4 = to_partner(theirs_4)
    pair_3 = functools.partial(pair, mine_3, other_3)
    pair_4 = functools.partial(pair, mine_4, other_4)
    far_low, far_high = added(
        [
            pair_3(0, low, (got_far, 0, low, 0)),
            pair_3(low, low, (got_far, low, low, 0)),
        ],
    )
    far_low, far_high = up(far_low), down(far_high)
    send_up, send_down = added(
        [pair_4(0, BLOCK, (got_up, 0, BLOCK, 0)), pair_4(BLOCK, BLOCK, (got_down, 0, BLOCK, 0))],
    )
    from_below, from_above = up(send_up), down(send_down)
    v_up, v_down = added(
        [
            pair_3(256, BLOCK, (got_near, 0, BLOCK, 0), (far_low, 0, low, 0)),
            pair_3(384, BLOCK, (got_near, BLOCK, BLOCK, 0), (far_high, 0, low, low)),
        ],
    )
    b_below, b_above = up(v_up), down(v_down)
    side_sum = added([pair_4(384, BLOCK, (got_up, BLOCK, BLOCK, 0), (from_above, 0, BLOCK, 0))])[0]
    got_side = to_side(side_sum)
    terms_b = [(mine_3, BLOCK), (other_3, BLOCK), (got_own, 0), (b_below, 0), (b_above, 0)]
    terms_a = [(mine_4, 256), (other_4, 256), (got_down, BLOCK), (from_below, 0), (got_side, 0)]
    comp_b, stepped_b = compress(1, factor, params, estimate, exponents, terms_b)
    left_b, right_b = around(comp_b, 1), around(comp_b, -1)
    comp_a, stepped_a = compress(0, factor, params, estimate, exponents, terms_a)
    left_a, right_a = around(comp_a, 1), around(comp_a, -1)
    own = (estimate, mixed_sum, edge_weight)
    base_b, rest_b, held = own_part(1, *own, comp_b, stepped_b, None, [comp_a])
    base_a, rest_a, new_estimate = own_part(0, *own, comp_a, stepped_a, held, [])
    outs = finish(1, edge_weight, base_b, rest_b, left_b, right_b, None, params.shape)
    new_params, new_mixed = finish(
        0, edge_weight, base_a, rest_a, left_a, right_a, outs, params.shape
    )
    return (new_params, new_estimate, new_mixed)


def solution(mesh):
    in_specs = (
        P("grp", "mem", None),
        P("grp", "mem", None),
        P("grp", "mem", None),
        P(("grp", "mem"), None),
        P(("grp", "mem"), None),
        P("grp", "mem"),
        P(),
    )
    out_specs = (P("grp", "mem", None), P("grp", "mem", None), P("grp", "mem", None))
    return jax.shard_map(
        on_device, mesh=mesh, in_specs=in_specs, out_specs=out_specs, check_vma=False
    )
```

```python
import functools
import math

import jax
import jax.numpy as jnp
from jax import lax
from jax.experimental import pallas as pl
from jax.experimental.pallas import tpu as pltpu
from jax.sharding import PartitionSpec as P


step_size = 0.5
mixing_rate = 0.4


f32 = jnp.float32
bf16 = jnp.bfloat16
ANY = pl.BlockSpec(memory_space=pl.ANY)
VMEM = pl.BlockSpec(memory_space=pltpu.VMEM)
BLOCK = 128
CHUNKS = 2
FIRST_LIMIT = 41


def member(z, x, c):
    return z * 4 + x * 2 + c


def moved(value, to):
    pairs = []
    for z in range(4):
        for x in range(2):
            for c in range(2):
                pairs.append((member(z, x, c), member(*to(z, x, c))))
    return lax.ppermute(value, "mem", pairs)


def to_partner(value):
    return moved(value, lambda z, x, c: (z, x, 1 - c))


def to_side(value):
    return moved(value, lambda z, x, c: (z, 1 - x, c))


def up(value):
    return moved(value, lambda z, x, c: ((z + 1) % 4, x, c))


def down(value):
    return moved(value, lambda z, x, c: ((z + 3) % 4, x, c))


def near_pairs(value):
    return lax.ppermute(value, "grp", [(g, g + 1 - 2 * (g % 2)) for g in range(8)])


def far_pairs(value):
    return lax.ppermute(value, "grp", [(g, (g + 7 + 2 * (g % 2)) % 8) for g in range(8)])


SENT_A = (((2, 0), (1, 1)), ((2, 1), (3, 0)))
KEPT_A = (((1, 0), (3, 1)), ((0, 0), (0, 1)))
SENT_B = (((1, 1), (3, 1)), ((2, 1), (0, 1)))
KEPT_B = (((2, 0), (0, 0)), ((1, 0), (3, 0)))


def products(activations, out_grads, side, tasks, after=()):
    depth, _ = activations.shape
    half = out_grads.shape[1] // 2
    piece = half // CHUNKS
    work = [(o, t) for t in range(len(tasks)) for o in (0, 1)]
    count = len(work)
    operands = [activations, out_grads, *after]
    shape = jax.ShapeDtypeStruct((len(tasks) * 2 * BLOCK, half), bf16)

    def body(*refs):
        a_ref, g_ref = refs[:2]
        out_refs = refs[len(operands) : len(operands) + 2]
        lhs = refs[-1]
        index = lax.axis_index("mem")
        z, x, c = index // 4, lax.rem(index // 2, 2), lax.rem(index, 2)
        for k, (own, t) in enumerate(work):
            for p, (dz, dx) in enumerate(tasks[t]):
                block = lax.rem(z + dz, 4) * 4 + lax.rem(x + dx, 2) * 2 + (c if own else 1 - c)
                source = pl.ds(pl.multiple_of(block * BLOCK, BLOCK), BLOCK)
                lhs[:, pl.ds((k * 2 + p) * BLOCK, BLOCK)] = a_ref[:, source]
        for j in range(CHUNKS):
            total = lax.dot_general(
                lhs[...],
                g_ref[:, pl.ds(side * half + j * piece, piece)],
                (((0,), (0,)), ((), ())),
                preferred_element_type=f32,
            ).astype(bf16)
            for k, (own, t) in enumerate(work):
                to = pl.ds(t * 2 * BLOCK, 2 * BLOCK)
                out_refs[own][to, pl.ds(j * piece, piece)] = total[k * 2 * BLOCK : (k + 1) * 2 * BLOCK]

    return pl.pallas_call(
        body,
        in_specs=[VMEM, VMEM] + [ANY] * len(after),
        out_specs=[VMEM, VMEM],
        out_shape=[shape] * 2,
        scratch_shapes=[pltpu.VMEM((depth, count * 2 * BLOCK), bf16)],
        compiler_params=pltpu.CompilerParams(vmem_limit_bytes=30 << 20),
        cost_estimate=pl.CostEstimate(
            flops=2 * count * 2 * BLOCK * half * depth,
            bytes_accessed=2 * (depth * half + count * 2 * BLOCK * (half + depth)),
            transcendentals=0,
        ),
    )(*operands)


def first_products(activations, out_grads, side, tasks, others):
    depth, rows = activations.shape
    width = out_grads.shape[1]
    half = width // 2
    piece = half // CHUNKS
    work = [(o, t) for t in range(len(tasks)) for o in (0, 1)]
    wanted = [(own, place) for own, t in work for place in tasks[t]]
    wanted += [(own, place) for own in (0, 1) for place in others]
    used = 2 * len(work)
    shape = jax.ShapeDtypeStruct((len(tasks) * 2 * BLOCK, half), bf16)

    def body(a_ref, g_ref, theirs, mine, a_all, g_all, lhs, a_sem, g_sem):
        index = lax.axis_index("mem")
        z, x, c = index // 4, lax.rem(index // 2, 2), lax.rem(index, 2)

        def columns(k):
            own, (dz, dx) = wanted[k]
            block = lax.rem(z + dz, 4) * 4 + lax.rem(x + dx, 2) * 2 + (c if own else 1 - c)
            return pl.ds(pl.multiple_of(block * BLOCK, BLOCK), BLOCK)

        def left(k):
            cut = columns(k)
            return pltpu.make_async_copy(a_ref.at[:, cut], a_all.at[:, cut], a_sem.at[k])

        def right(h, j):
            cut = pl.ds(h * half + j * piece, piece)
            return pltpu.make_async_copy(g_ref.at[:, cut], g_all.at[:, cut], g_sem.at[h, j])

        for k in range(used):
            left(k).start()
        for j in range(CHUNKS):
            right(side, j).start()
        for k in range(used, len(wanted)):
            left(k).start()
        for j in range(CHUNKS):
            right(1 - side, j).start()
        for k in range(used):
            left(k).wait()
            lhs[:, pl.ds(k * BLOCK, BLOCK)] = a_all[:, columns(k)]
        for j in range(CHUNKS):
            right(side, j).wait()
            total = lax.dot_general(
                lhs[...],
                g_all[:, pl.ds(side * half + j * piece, piece)],
                (((0,), (0,)), ((), ())),
                preferred_element_type=f32,
            ).astype(bf16)
            for k, (own, t) in enumerate(work):
                to = pl.ds(t * 2 * BLOCK, 2 * BLOCK)
                out = (theirs, mine)[own]
                out[to, pl.ds(j * piece, piece)] = total[k * 2 * BLOCK : (k + 1) * 2 * BLOCK]
        for k in range(used, len(wanted)):
            left(k).wait()
        for j in range(CHUNKS):
            right(1 - side, j).wait()

    return pl.pallas_call(
        body,
        in_specs=[ANY, ANY],
        out_specs=[VMEM] * 4,
        out_shape=[
            shape,
            shape,
            jax.ShapeDtypeStruct(activations.shape, bf16),
            jax.ShapeDtypeStruct(out_grads.shape, bf16),
        ],
        scratch_shapes=[
            pltpu.VMEM((depth, used * BLOCK), bf16),
            pltpu.SemaphoreType.DMA((len(wanted),)),
            pltpu.SemaphoreType.DMA((2, CHUNKS)),
        ],
        compiler_params=pltpu.CompilerParams(vmem_limit_bytes=FIRST_LIMIT << 20),
        cost_estimate=pl.CostEstimate(
            flops=2 * used * BLOCK * half * depth,
            bytes_accessed=4 * depth * (rows + width),
            transcendentals=0,
        ),
    )(activations, out_grads)


def added(outs, steps=1):
    operands, in_specs = [], []
    width = outs[0][1][0][0].shape[1]
    piece = width // steps
    for _, terms in outs:
        for value, start, size, _ in terms:
            operands.append(value)
            in_specs.append(
                pl.BlockSpec((size, piece), functools.partial(lambda s, i: (s, i), start // size))
            )

    def body(*refs):
        at = 0
        for (rows, terms), out in zip(outs, refs[len(operands) :]):
            edges = sorted({0, rows} | {t[3] for t in terms} | {t[3] + t[2] for t in terms})
            for low, high in zip(edges, edges[1:]):
                total = None
                for k, (_, _, size, place) in enumerate(terms):
                    if place <= low and high <= place + size:
                        value = refs[at + k][low - place : high - place, :].astype(f32)
                        total = value if total is None else total + value
                out[low:high, :] = total.astype(bf16)
            at += len(terms)

    return pl.pallas_call(
        body,
        grid=(steps,),
        in_specs=in_specs,
        out_specs=[pl.BlockSpec((rows, piece), lambda i: (0, i)) for rows, _ in outs],
        out_shape=[jax.ShapeDtypeStruct((rows, width), bf16) for rows, _ in outs],
        compiler_params=pltpu.CompilerParams(vmem_limit_bytes=24 << 20),
        cost_estimate=pl.CostEstimate(flops=1 << 20, bytes_accessed=1 << 20, transcendentals=0),
    )(*operands)


def kernel(body, operands, in_specs, out_specs, out_shape, aliases, steps=1):
    return pl.pallas_call(
        body,
        grid=(steps,),
        in_specs=in_specs,
        out_specs=out_specs,
        out_shape=out_shape,
        input_output_aliases=aliases,
        compiler_params=pltpu.CompilerParams(vmem_limit_bytes=16 << 20),
        cost_estimate=pl.CostEstimate(flops=2 << 20, bytes_accessed=3 << 20, transcendentals=0),
    )(*operands)


SMEM = pl.BlockSpec(memory_space=pltpu.SMEM)


def compress(side, factor, params, estimate, exponents, terms):
    rows, width = params.shape[1:]
    half = width // 2
    span = rows // exponents.shape[1]
    big = pl.BlockSpec((1, rows, half), lambda i: (0, 0, side))
    flat = pl.BlockSpec((rows, half), lambda i: (0, 0))
    operands = [exponents, params, estimate]
    in_specs = [SMEM, big, big]
    for value, start in terms:
        operands.append(value)
        in_specs.append(pl.BlockSpec((rows, half), lambda i, s=start // rows: (s, 0)))

    def body(*refs):
        e_ref, p_ref, s_ref = refs[:3]
        comp_ref, stepped_ref = refs[len(operands) :]
        for part in range(rows // span):
            exponent = e_ref[0, part]
            scale = jnp.left_shift(jnp.int32(1), exponent).astype(f32)
            inverse = jnp.left_shift(jnp.int32(1), 24 - exponent).astype(f32) * (2.0**-24)
            cut = slice(part * span, (part + 1) * span)
            gradient = refs[3][cut, :].astype(f32)
            for k in range(1, len(terms)):
                gradient = gradient + refs[3 + k][cut, :].astype(f32)
            stepped = p_ref[0, cut, :] - factor * gradient
            change = stepped - s_ref[0, cut, :]
            levels = jnp.clip(change * inverse, -1.0, 1.0).astype(bf16)
            comp_ref[cut, :] = (levels.astype(f32) * scale).astype(bf16)
            stepped_ref[cut, :] = stepped

    shapes = [jax.ShapeDtypeStruct((rows, half), bf16), jax.ShapeDtypeStruct((rows, half), f32)]
    return kernel(body, operands, in_specs, [flat, flat], shapes, {})


def own_part(side, estimate, mixed_sum, edge_weight, compressed, stepped, held, after):
    rows, width = estimate.shape[1:]
    half = width // 2
    big = pl.BlockSpec((1, rows, half), lambda i: (0, 0, side))
    flat = pl.BlockSpec((rows, half), lambda i: (0, 0))
    operands = [edge_weight, estimate, mixed_sum, compressed, stepped]
    in_specs = [SMEM, big, big, flat, flat]
    aliases = {}
    if held is not None:
        aliases = {len(operands): 2}
        operands.append(held)
        in_specs.append(ANY)
    operands += after
    in_specs += [ANY] * len(after)

    def body(*refs):
        w_ref, s_ref, m_ref, c_ref, p_ref = refs[:5]
        base_ref, rest_ref, est_ref = refs[len(operands) :]
        group = lax.axis_index("grp")
        right, left = w_ref[group], w_ref[lax.rem(group + 7, 8)]
        own = c_ref[...].astype(f32)
        new = s_ref[0] + own
        base_ref[...] = m_ref[0] + (1.0 - left - right) * own
        rest_ref[...] = p_ref[...] - mixing_rate * new
        est_ref[0] = new

    shapes = [jax.ShapeDtypeStruct((rows, half), f32)] * 2
    shapes.append(jax.ShapeDtypeStruct(estimate.shape, f32))
    return kernel(body, operands, in_specs, [flat, flat, big], shapes, aliases)


def finish(side, edge_weight, base, rest, from_far, from_near, held, shape):
    rows, width = shape[1:]
    half = width // 2
    piece = half // 2
    big = pl.BlockSpec((1, rows, piece), lambda i: (0, 0, side * 2 + i))
    flat = pl.BlockSpec((rows, piece), lambda i: (0, i))
    operands = [edge_weight, base, rest, from_far, from_near]
    in_specs = [SMEM, flat, flat, flat, flat]
    aliases = {}
    if held is not None:
        aliases = {len(operands): 0, len(operands) + 1: 1}
        operands += list(held)
        in_specs += [ANY, ANY]

    def body(*refs):
        w_ref, base_ref, rest_ref, far_ref, near_ref = refs[:5]
        new_params, new_mixed = refs[len(operands) :]
        group = lax.axis_index("grp")
        right, left = w_ref[group], w_ref[lax.rem(group + 7, 8)]
        odd = lax.rem(group, 2) == 1
        mixed = base_ref[...] + jnp.where(odd, right, left) * far_ref[...].astype(f32)
        mixed = mixed + jnp.where(odd, left, right) * near_ref[...].astype(f32)
        new_mixed[0] = mixed
        new_params[0] = rest_ref[...] + mixing_rate * mixed

    shapes = [jax.ShapeDtypeStruct(shape, f32)] * 2
    return kernel(body, operands, in_specs, [big, big], shapes, aliases, 2)


def on_device(params, estimate, mixed_sum, activations, out_grads, exponents, edge_weight):
    factor = step_size / math.sqrt(lax.axis_size("mem") * activations.shape[0])
    low = BLOCK // 2
    theirs_1, mine_1, activations, out_grads = first_products(
        activations, out_grads, 0, SENT_A, [place for task in KEPT_A for place in task]
    )
    other_1 = to_partner(theirs_1)
    theirs_2, mine_2 = products(activations, out_grads, 1, SENT_B, [theirs_1])
    other_2 = to_partner(theirs_2)

    def pair(mine, other, start, size, *more):
        return (size, [(mine, start, size, 0), (other, start, size, 0), *more])

    pair_1 = functools.partial(pair, mine_1, other_1)
    pair_2 = functools.partial(pair, mine_2, other_2)
    a_up, a_down = added([pair_1(0, 256), pair_1(256, 256)])
    got_up, got_down = up(a_up), down(a_down)
    b_near, b_far, b_own = added([pair_2(0, 256), pair_2(256, 128), pair_2(384, 128)])
    got_far = to_side(b_far)
    got_near, got_own = to_side(b_near), to_side(b_own)
    theirs_3, mine_3 = products(activations, out_grads, 1, KEPT_B, [a_up, b_far])
    other_3 = to_partner(theirs_3)
    theirs_4, mine_4 = products(activations, out_grads, 0, KEPT_A, [theirs_3])
    other_4 = to_partner(theirs_4)
    pair_3 = functools.partial(pair, mine_3, other_3)
    pair_4 = functools.partial(pair, mine_4, other_4)
    far_low, far_high = added(
        [
            pair_3(0, low, (got_far, 0, low, 0)),
            pair_3(low, low, (got_far, low, low, 0)),
        ],
    )
    far_low, far_high = up(far_low), down(far_high)
    send_down = added([pair_4(BLOCK, BLOCK, (got_down, 0, BLOCK, 0))])[0]
    send_up = added([pair_4(0, BLOCK, (got_up, 0, BLOCK, 0))])[0]
    from_below, from_above = up(send_up), down(send_down)
    v_up, v_down = added(
        [
            pair_3(256, BLOCK, (got_near, 0, BLOCK, 0), (far_low, 0, low, 0)),
            pair_3(384, BLOCK, (got_near, BLOCK, BLOCK, 0), (far_high, 0, low, low)),
        ],
    )
    b_below, b_above = up(v_up), down(v_down)
    side_sum = added([pair_4(384, BLOCK, (got_up, BLOCK, BLOCK, 0), (from_above, 0, BLOCK, 0))])[0]
    got_side = to_side(side_sum)
    terms_b = [(mine_3, BLOCK), (other_3, BLOCK), (got_own, 0), (b_below, 0), (b_above, 0)]
    terms_a = [(mine_4, 256), (other_4, 256), (got_down, BLOCK), (from_below, 0), (got_side, 0)]
    comp_b, stepped_b = compress(1, factor, params, estimate, exponents, terms_b)
    far_b, near_b = far_pairs(comp_b), near_pairs(comp_b)
    comp_a, stepped_a = compress(0, factor, params, estimate, exponents, terms_a)
    far_a, near_a = far_pairs(comp_a), near_pairs(comp_a)
    own = (estimate, mixed_sum, edge_weight)
    base_b, rest_b, held = own_part(1, *own, comp_b, stepped_b, None, [comp_a])
    base_a, rest_a, new_estimate = own_part(0, *own, comp_a, stepped_a, held, [])
    outs = finish(1, edge_weight, base_b, rest_b, far_b, near_b, None, params.shape)
    new_params, new_mixed = finish(
        0, edge_weight, base_a, rest_a, far_a, near_a, outs, params.shape
    )
    return (new_params, new_estimate, new_mixed)


def solution(mesh):
    in_specs = (
        P("grp", "mem", None),
        P("grp", "mem", None),
        P("grp", "mem", None),
        P(("grp", "mem"), None),
        P(("grp", "mem"), None),
        P("grp", "mem"),
        P(),
    )
    out_specs = (P("grp", "mem", None), P("grp", "mem", None), P("grp", "mem", None))
    return jax.shard_map(
        on_device, mesh=mesh, in_specs=in_specs, out_specs=out_specs, check_vma=False
    )
```

```python
import functools
import math

import jax
import jax.numpy as jnp
from jax import lax
from jax.experimental import pallas as pl
from jax.experimental.pallas import tpu as pltpu
from jax.sharding import PartitionSpec as P


step_size = 0.5
mixing_rate = 0.4


f32 = jnp.float32
bf16 = jnp.bfloat16
ANY = pl.BlockSpec(memory_space=pl.ANY)
VMEM = pl.BlockSpec(memory_space=pltpu.VMEM)
BLOCK = 128
CHUNKS = 2
FIRST_LIMIT = 41


def member(z, x, c):
    return z * 4 + x * 2 + c


def moved(value, to):
    pairs = []
    for z in range(4):
        for x in range(2):
            for c in range(2):
                pairs.append((member(z, x, c), member(*to(z, x, c))))
    return lax.ppermute(value, "mem", pairs)


def to_partner(value):
    return moved(value, lambda z, x, c: (z, x, 1 - c))


def to_side(value):
    return moved(value, lambda z, x, c: (z, 1 - x, c))


def up(value):
    return moved(value, lambda z, x, c: ((z + 1) % 4, x, c))


def down(value):
    return moved(value, lambda z, x, c: ((z + 3) % 4, x, c))


def near_pairs(value):
    return lax.ppermute(value, "grp", [(g, g + 1 - 2 * (g % 2)) for g in range(8)])


def far_pairs(value):
    return lax.ppermute(value, "grp", [(g, (g + 7 + 2 * (g % 2)) % 8) for g in range(8)])


SENT_A = (((2, 0), (1, 1)), ((2, 1), (3, 0)))
KEPT_A = (((1, 0), (3, 1)), ((0, 0), (0, 1)))
SENT_B = (((1, 1), (3, 1)), ((2, 1), (0, 1)))
KEPT_B = (((2, 0), (0, 0)), ((1, 0), (3, 0)))


def products(activations, out_grads, side, tasks, after=()):
    depth, _ = activations.shape
    half = out_grads.shape[1] // 2
    piece = half // CHUNKS
    work = [(o, t) for t in range(len(tasks)) for o in (0, 1)]
    count = len(work)
    operands = [activations, out_grads, *after]
    shape = jax.ShapeDtypeStruct((len(tasks) * 2 * BLOCK, half), bf16)

    def body(*refs):
        a_ref, g_ref = refs[:2]
        out_refs = refs[len(operands) : len(operands) + 2]
        lhs = refs[-1]
        index = lax.axis_index("mem")
        z, x, c = index // 4, lax.rem(index // 2, 2), lax.rem(index, 2)
        for k, (own, t) in enumerate(work):
            for p, (dz, dx) in enumerate(tasks[t]):
                block = lax.rem(z + dz, 4) * 4 + lax.rem(x + dx, 2) * 2 + (c if own else 1 - c)
                source = pl.ds(pl.multiple_of(block * BLOCK, BLOCK), BLOCK)
                lhs[:, pl.ds((k * 2 + p) * BLOCK, BLOCK)] = a_ref[:, source]
        for j in range(CHUNKS):
            total = lax.dot_general(
                lhs[...],
                g_ref[:, pl.ds(side * half + j * piece, piece)],
                (((0,), (0,)), ((), ())),
                preferred_element_type=f32,
            ).astype(bf16)
            for k, (own, t) in enumerate(work):
                to = pl.ds(t * 2 * BLOCK, 2 * BLOCK)
                out_refs[own][to, pl.ds(j * piece, piece)] = total[k * 2 * BLOCK : (k + 1) * 2 * BLOCK]

    return pl.pallas_call(
        body,
        in_specs=[VMEM, VMEM] + [ANY] * len(after),
        out_specs=[VMEM, VMEM],
        out_shape=[shape] * 2,
        scratch_shapes=[pltpu.VMEM((depth, count * 2 * BLOCK), bf16)],
        compiler_params=pltpu.CompilerParams(vmem_limit_bytes=30 << 20),
        cost_estimate=pl.CostEstimate(
            flops=2 * count * 2 * BLOCK * half * depth,
            bytes_accessed=2 * (depth * half + count * 2 * BLOCK * (half + depth)),
            transcendentals=0,
        ),
    )(*operands)


def first_products(activations, out_grads, side, tasks, others):
    depth, rows = activations.shape
    width = out_grads.shape[1]
    half = width // 2
    piece = half // CHUNKS
    work = [(o, t) for t in range(len(tasks)) for o in (0, 1)]
    wanted = [(own, place) for own, t in work for place in tasks[t]]
    wanted += [(own, place) for own in (0, 1) for place in others]
    used = 2 * len(work)
    shape = jax.ShapeDtypeStruct((len(tasks) * 2 * BLOCK, half), bf16)

    def body(a_ref, g_ref, theirs, mine, a_all, g_all, lhs, a_sem, g_sem):
        index = lax.axis_index("mem")
        z, x, c = index // 4, lax.rem(index // 2, 2), lax.rem(index, 2)

        def columns(k):
            own, (dz, dx) = wanted[k]
            block = lax.rem(z + dz, 4) * 4 + lax.rem(x + dx, 2) * 2 + (c if own else 1 - c)
            return pl.ds(pl.multiple_of(block * BLOCK, BLOCK), BLOCK)

        def left(k):
            cut = columns(k)
            return pltpu.make_async_copy(a_ref.at[:, cut], a_all.at[:, cut], a_sem.at[k])

        def right(h, j):
            cut = pl.ds(h * half + j * piece, piece)
            return pltpu.make_async_copy(g_ref.at[:, cut], g_all.at[:, cut], g_sem.at[h, j])

        for k in range(used):
            left(k).start()
        for j in range(CHUNKS):
            right(side, j).start()
        for k in range(used, len(wanted)):
            left(k).start()
        for j in range(CHUNKS):
            right(1 - side, j).start()
        for k in range(used):
            left(k).wait()
            lhs[:, pl.ds(k * BLOCK, BLOCK)] = a_all[:, columns(k)]
        for j in range(CHUNKS):
            right(side, j).wait()
            total = lax.dot_general(
                lhs[...],
                g_all[:, pl.ds(side * half + j * piece, piece)],
                (((0,), (0,)), ((), ())),
                preferred_element_type=f32,
            ).astype(bf16)
            for k, (own, t) in enumerate(work):
                to = pl.ds(t * 2 * BLOCK, 2 * BLOCK)
                out = (theirs, mine)[own]
                out[to, pl.ds(j * piece, piece)] = total[k * 2 * BLOCK : (k + 1) * 2 * BLOCK]
        for k in range(used, len(wanted)):
            left(k).wait()
        for j in range(CHUNKS):
            right(1 - side, j).wait()

    return pl.pallas_call(
        body,
        in_specs=[ANY, ANY],
        out_specs=[VMEM] * 4,
        out_shape=[
            shape,
            shape,
            jax.ShapeDtypeStruct(activations.shape, bf16),
            jax.ShapeDtypeStruct(out_grads.shape, bf16),
        ],
        scratch_shapes=[
            pltpu.VMEM((depth, used * BLOCK), bf16),
            pltpu.SemaphoreType.DMA((len(wanted),)),
            pltpu.SemaphoreType.DMA((2, CHUNKS)),
        ],
        compiler_params=pltpu.CompilerParams(vmem_limit_bytes=FIRST_LIMIT << 20),
        cost_estimate=pl.CostEstimate(
            flops=2 * used * BLOCK * half * depth,
            bytes_accessed=4 * depth * (rows + width),
            transcendentals=0,
        ),
    )(activations, out_grads)


def added(outs, steps=1):
    operands, in_specs = [], []
    width = outs[0][1][0][0].shape[1]
    piece = width // steps
    for _, terms in outs:
        for value, start, size, _ in terms:
            operands.append(value)
            in_specs.append(
                pl.BlockSpec((size, piece), functools.partial(lambda s, i: (s, i), start // size))
            )

    def body(*refs):
        at = 0
        for (rows, terms), out in zip(outs, refs[len(operands) :]):
            edges = sorted({0, rows} | {t[3] for t in terms} | {t[3] + t[2] for t in terms})
            for low, high in zip(edges, edges[1:]):
                total = None
                for k, (_, _, size, place) in enumerate(terms):
                    if place <= low and high <= place + size:
                        value = refs[at + k][low - place : high - place, :].astype(f32)
                        total = value if total is None else total + value
                out[low:high, :] = total.astype(bf16)
            at += len(terms)

    return pl.pallas_call(
        body,
        grid=(steps,),
        in_specs=in_specs,
        out_specs=[pl.BlockSpec((rows, piece), lambda i: (0, i)) for rows, _ in outs],
        out_shape=[jax.ShapeDtypeStruct((rows, width), bf16) for rows, _ in outs],
        compiler_params=pltpu.CompilerParams(vmem_limit_bytes=24 << 20),
        cost_estimate=pl.CostEstimate(flops=1 << 20, bytes_accessed=1 << 20, transcendentals=0),
    )(*operands)


def kernel(body, operands, in_specs, out_specs, out_shape, aliases, steps=1):
    return pl.pallas_call(
        body,
        grid=(steps,),
        in_specs=in_specs,
        out_specs=out_specs,
        out_shape=out_shape,
        input_output_aliases=aliases,
        compiler_params=pltpu.CompilerParams(vmem_limit_bytes=16 << 20),
        cost_estimate=pl.CostEstimate(flops=2 << 20, bytes_accessed=3 << 20, transcendentals=0),
    )(*operands)


SMEM = pl.BlockSpec(memory_space=pltpu.SMEM)


def compress(side, factor, params, estimate, exponents, terms):
    rows, width = params.shape[1:]
    half = width // 2
    span = rows // exponents.shape[1]
    big = pl.BlockSpec((1, rows, half), lambda i: (0, 0, side))
    flat = pl.BlockSpec((rows, half), lambda i: (0, 0))
    operands = [exponents, params, estimate]
    in_specs = [SMEM, big, big]
    for value, start in terms:
        operands.append(value)
        in_specs.append(pl.BlockSpec((rows, half), lambda i, s=start // rows: (s, 0)))

    def body(*refs):
        e_ref, p_ref, s_ref = refs[:3]
        comp_ref, stepped_ref = refs[len(operands) :]
        for part in range(rows // span):
            exponent = e_ref[0, part]
            scale = jnp.left_shift(jnp.int32(1), exponent).astype(f32)
            inverse = jnp.left_shift(jnp.int32(1), 24 - exponent).astype(f32) * (2.0**-24)
            cut = slice(part * span, (part + 1) * span)
            gradient = refs[3][cut, :].astype(f32)
            for k in range(1, len(terms)):
                gradient = gradient + refs[3 + k][cut, :].astype(f32)
            stepped = p_ref[0, cut, :] - factor * gradient
            change = stepped - s_ref[0, cut, :]
            levels = jnp.clip(change * inverse, -1.0, 1.0).astype(bf16)
            comp_ref[cut, :] = (levels.astype(f32) * scale).astype(bf16)
            stepped_ref[cut, :] = stepped

    shapes = [jax.ShapeDtypeStruct((rows, half), bf16), jax.ShapeDtypeStruct((rows, half), f32)]
    return kernel(body, operands, in_specs, [flat, flat], shapes, {})


def own_part(side, estimate, mixed_sum, edge_weight, compressed, stepped, held, after):
    rows, width = estimate.shape[1:]
    half = width // 2
    big = pl.BlockSpec((1, rows, half), lambda i: (0, 0, side))
    flat = pl.BlockSpec((rows, half), lambda i: (0, 0))
    operands = [edge_weight, estimate, mixed_sum, compressed, stepped]
    in_specs = [SMEM, big, big, flat, flat]
    aliases = {}
    if held is not None:
        aliases = {len(operands): 2}
        operands.append(held)
        in_specs.append(ANY)
    operands += after
    in_specs += [ANY] * len(after)

    def body(*refs):
        w_ref, s_ref, m_ref, c_ref, p_ref = refs[:5]
        base_ref, rest_ref, est_ref = refs[len(operands) :]
        group = lax.axis_index("grp")
        right, left = w_ref[group], w_ref[lax.rem(group + 7, 8)]
        own = c_ref[...].astype(f32)
        new = s_ref[0] + own
        base_ref[...] = m_ref[0] + (1.0 - left - right) * own
        rest_ref[...] = p_ref[...] - mixing_rate * new
        est_ref[0] = new

    shapes = [jax.ShapeDtypeStruct((rows, half), f32)] * 2
    shapes.append(jax.ShapeDtypeStruct(estimate.shape, f32))
    return kernel(body, operands, in_specs, [flat, flat, big], shapes, aliases)


def finish(side, edge_weight, base, rest, from_far, from_near, held, shape):
    rows, width = shape[1:]
    half = width // 2
    piece = half // 2
    big = pl.BlockSpec((1, rows, piece), lambda i: (0, 0, side * 2 + i))
    flat = pl.BlockSpec((rows, piece), lambda i: (0, i))
    operands = [edge_weight, base, rest, from_far, from_near]
    in_specs = [SMEM, flat, flat, flat, flat]
    aliases = {}
    if held is not None:
        aliases = {len(operands): 0, len(operands) + 1: 1}
        operands += list(held)
        in_specs += [ANY, ANY]

    def body(*refs):
        w_ref, base_ref, rest_ref, far_ref, near_ref = refs[:5]
        new_params, new_mixed = refs[len(operands) :]
        group = lax.axis_index("grp")
        right, left = w_ref[group], w_ref[lax.rem(group + 7, 8)]
        odd = lax.rem(group, 2) == 1
        mixed = base_ref[...] + jnp.where(odd, right, left) * far_ref[...].astype(f32)
        mixed = mixed + jnp.where(odd, left, right) * near_ref[...].astype(f32)
        new_mixed[0] = mixed
        new_params[0] = rest_ref[...] + mixing_rate * mixed

    shapes = [jax.ShapeDtypeStruct(shape, f32)] * 2
    return kernel(body, operands, in_specs, [big, big], shapes, aliases, 2)


def on_device(params, estimate, mixed_sum, activations, out_grads, exponents, edge_weight):
    factor = step_size / math.sqrt(lax.axis_size("mem") * activations.shape[0])
    low = BLOCK // 2
    theirs_1, mine_1, activations, out_grads = first_products(
        activations, out_grads, 0, SENT_A, [place for task in KEPT_A for place in task]
    )
    other_1 = to_partner(theirs_1)
    theirs_2, mine_2 = products(activations, out_grads, 1, SENT_B, [theirs_1])
    other_2 = to_partner(theirs_2)

    def pair(mine, other, start, size, *more):
        return (size, [(mine, start, size, 0), (other, start, size, 0), *more])

    pair_1 = functools.partial(pair, mine_1, other_1)
    pair_2 = functools.partial(pair, mine_2, other_2)
    a_up, a_down = added([pair_1(0, 256), pair_1(256, 256)])
    got_up, got_down = up(a_up), down(a_down)
    b_above, b_below, b_far, b_own = added([pair_2(k * BLOCK, BLOCK) for k in range(4)])
    got_far = to_side(b_far)
    got_above, got_below = to_side(b_above), to_side(b_below)
    got_own = to_side(b_own)
    theirs_3, mine_3 = products(activations, out_grads, 1, KEPT_B, [a_up, b_far])
    other_3 = to_partner(theirs_3)
    theirs_4, mine_4 = products(activations, out_grads, 0, KEPT_A, [theirs_3])
    other_4 = to_partner(theirs_4)
    pair_3 = functools.partial(pair, mine_3, other_3)
    pair_4 = functools.partial(pair, mine_4, other_4)
    far_low, far_high = added(
        [
            pair_3(0, low, (got_far, 0, low, 0)),
            pair_3(low, low, (got_far, low, low, 0)),
        ],
    )
    far_low, far_high = up(far_low), down(far_high)
    send_down = added([pair_4(BLOCK, BLOCK, (got_down, 0, BLOCK, 0))])[0]
    send_up = added([pair_4(0, BLOCK, (got_up, 0, BLOCK, 0))])[0]
    from_below, from_above = up(send_up), down(send_down)
    v_up = added([pair_3(256, BLOCK, (got_above, 0, BLOCK, 0), (far_low, 0, low, 0))])[0]
    v_down = added([pair_3(384, BLOCK, (got_below, 0, BLOCK, 0), (far_high, 0, low, low))])[0]
    b_below, b_above = up(v_up), down(v_down)
    side_sum = added([pair_4(384, BLOCK, (got_up, BLOCK, BLOCK, 0), (from_above, 0, BLOCK, 0))])[0]
    got_side = to_side(side_sum)
    terms_b = [(mine_3, BLOCK), (other_3, BLOCK), (got_own, 0), (b_below, 0), (b_above, 0)]
    terms_a = [(mine_4, 256), (other_4, 256), (got_down, BLOCK), (from_below, 0), (got_side, 0)]
    comp_b, stepped_b = compress(1, factor, params, estimate, exponents, terms_b)
    far_b, near_b = far_pairs(comp_b), near_pairs(comp_b)
    comp_a, stepped_a = compress(0, factor, params, estimate, exponents, terms_a)
    far_a, near_a = far_pairs(comp_a), near_pairs(comp_a)
    own = (estimate, mixed_sum, edge_weight)
    base_b, rest_b, held = own_part(1, *own, comp_b, stepped_b, None, [comp_a])
    base_a, rest_a, new_estimate = own_part(0, *own, comp_a, stepped_a, held, [])
    outs = finish(1, edge_weight, base_b, rest_b, far_b, near_b, None, params.shape)
    new_params, new_mixed = finish(
        0, edge_weight, base_a, rest_a, far_a, near_a, outs, params.shape
    )
    return (new_params, new_estimate, new_mixed)


def solution(mesh):
    in_specs = (
        P("grp", "mem", None),
        P("grp", "mem", None),
        P("grp", "mem", None),
        P(("grp", "mem"), None),
        P(("grp", "mem"), None),
        P("grp", "mem"),
        P(),
    )
    out_specs = (P("grp", "mem", None), P("grp", "mem", None), P("grp", "mem", None))
    return jax.shard_map(
        on_device, mesh=mesh, in_specs=in_specs, out_specs=out_specs, check_vma=False
    )
```

```python
import functools
import math

import jax
import jax.numpy as jnp
from jax import lax
from jax.experimental import pallas as pl
from jax.experimental.pallas import tpu as pltpu
from jax.sharding import PartitionSpec as P


step_size = 0.5
mixing_rate = 0.4


f32 = jnp.float32
bf16 = jnp.bfloat16
ANY = pl.BlockSpec(memory_space=pl.ANY)
VMEM = pl.BlockSpec(memory_space=pltpu.VMEM)
BLOCK = 128
CHUNKS = 2
FIRST_LIMIT = 41


def member(z, x, c):
    return z * 4 + x * 2 + c


def moved(value, to):
    pairs = []
    for z in range(4):
        for x in range(2):
            for c in range(2):
                pairs.append((member(z, x, c), member(*to(z, x, c))))
    return lax.ppermute(value, "mem", pairs)


def to_partner(value):
    return moved(value, lambda z, x, c: (z, x, 1 - c))


def to_side(value):
    return moved(value, lambda z, x, c: (z, 1 - x, c))


def up(value):
    return moved(value, lambda z, x, c: ((z + 1) % 4, x, c))


def down(value):
    return moved(value, lambda z, x, c: ((z + 3) % 4, x, c))


def near_pairs(value):
    return lax.ppermute(value, "grp", [(g, g + 1 - 2 * (g % 2)) for g in range(8)])


def far_pairs(value):
    return lax.ppermute(value, "grp", [(g, (g + 7 + 2 * (g % 2)) % 8) for g in range(8)])


SENT_A = (((2, 0), (1, 1)), ((2, 1), (3, 0)))
KEPT_A = (((1, 0), (3, 1)), ((0, 0), (0, 1)))
SENT_B = (((1, 1), (3, 1)), ((2, 1), (0, 1)))
KEPT_B = (((2, 0), (0, 0)), ((1, 0), (3, 0)))


def products(activations, out_grads, side, tasks, after=()):
    depth, _ = activations.shape
    half = out_grads.shape[1] // 2
    piece = half // CHUNKS
    work = [(o, t) for t in range(len(tasks)) for o in (0, 1)]
    count = len(work)
    operands = [activations, out_grads, *after]
    shape = jax.ShapeDtypeStruct((len(tasks) * 2 * BLOCK, half), bf16)

    def body(*refs):
        a_ref, g_ref = refs[:2]
        out_refs = refs[len(operands) : len(operands) + 2]
        lhs = refs[-1]
        index = lax.axis_index("mem")
        z, x, c = index // 4, lax.rem(index // 2, 2), lax.rem(index, 2)
        for k, (own, t) in enumerate(work):
            for p, (dz, dx) in enumerate(tasks[t]):
                block = lax.rem(z + dz, 4) * 4 + lax.rem(x + dx, 2) * 2 + (c if own else 1 - c)
                source = pl.ds(pl.multiple_of(block * BLOCK, BLOCK), BLOCK)
                lhs[:, pl.ds((k * 2 + p) * BLOCK, BLOCK)] = a_ref[:, source]
        for j in range(CHUNKS):
            total = lax.dot_general(
                lhs[...],
                g_ref[:, pl.ds(side * half + j * piece, piece)],
                (((0,), (0,)), ((), ())),
                preferred_element_type=f32,
            ).astype(bf16)
            for k, (own, t) in enumerate(work):
                to = pl.ds(t * 2 * BLOCK, 2 * BLOCK)
                out_refs[own][to, pl.ds(j * piece, piece)] = total[k * 2 * BLOCK : (k + 1) * 2 * BLOCK]

    return pl.pallas_call(
        body,
        in_specs=[VMEM, VMEM] + [ANY] * len(after),
        out_specs=[VMEM, VMEM],
        out_shape=[shape] * 2,
        scratch_shapes=[pltpu.VMEM((depth, count * 2 * BLOCK), bf16)],
        compiler_params=pltpu.CompilerParams(vmem_limit_bytes=30 << 20),
        cost_estimate=pl.CostEstimate(
            flops=2 * count * 2 * BLOCK * half * depth,
            bytes_accessed=2 * (depth * half + count * 2 * BLOCK * (half + depth)),
            transcendentals=0,
        ),
    )(*operands)


def first_products(activations, out_grads, side, tasks, others):
    depth, rows = activations.shape
    width = out_grads.shape[1]
    half = width // 2
    piece = half // CHUNKS
    work = [(o, t) for t in range(len(tasks)) for o in (0, 1)]
    wanted = [(own, place) for own, t in work for place in tasks[t]]
    wanted += [(own, place) for own in (0, 1) for place in others]
    used = 2 * len(work)
    shape = jax.ShapeDtypeStruct((len(tasks) * 2 * BLOCK, half), bf16)

    def body(a_ref, g_ref, theirs, mine, a_all, g_all, lhs, a_sem, g_sem):
        index = lax.axis_index("mem")
        z, x, c = index // 4, lax.rem(index // 2, 2), lax.rem(index, 2)

        def columns(k):
            own, (dz, dx) = wanted[k]
            block = lax.rem(z + dz, 4) * 4 + lax.rem(x + dx, 2) * 2 + (c if own else 1 - c)
            return pl.ds(pl.multiple_of(block * BLOCK, BLOCK), BLOCK)

        def left(k):
            cut = columns(k)
            return pltpu.make_async_copy(a_ref.at[:, cut], a_all.at[:, cut], a_sem.at[k])

        def right(h, j):
            cut = pl.ds(h * half + j * piece, piece)
            return pltpu.make_async_copy(g_ref.at[:, cut], g_all.at[:, cut], g_sem.at[h, j])

        for k in range(used):
            left(k).start()
        for j in range(CHUNKS):
            right(side, j).start()
        for k in range(used, len(wanted)):
            left(k).start()
        for j in range(CHUNKS):
            right(1 - side, j).start()
        for k in range(used):
            left(k).wait()
            lhs[:, pl.ds(k * BLOCK, BLOCK)] = a_all[:, columns(k)]
        for j in range(CHUNKS):
            right(side, j).wait()
            total = lax.dot_general(
                lhs[...],
                g_all[:, pl.ds(side * half + j * piece, piece)],
                (((0,), (0,)), ((), ())),
                preferred_element_type=f32,
            ).astype(bf16)
            for k, (own, t) in enumerate(work):
                to = pl.ds(t * 2 * BLOCK, 2 * BLOCK)
                out = (theirs, mine)[own]
                out[to, pl.ds(j * piece, piece)] = total[k * 2 * BLOCK : (k + 1) * 2 * BLOCK]
        for k in range(used, len(wanted)):
            left(k).wait()
        for j in range(CHUNKS):
            right(1 - side, j).wait()

    return pl.pallas_call(
        body,
        in_specs=[ANY, ANY],
        out_specs=[VMEM] * 4,
        out_shape=[
            shape,
            shape,
            jax.ShapeDtypeStruct(activations.shape, bf16),
            jax.ShapeDtypeStruct(out_grads.shape, bf16),
        ],
        scratch_shapes=[
            pltpu.VMEM((depth, used * BLOCK), bf16),
            pltpu.SemaphoreType.DMA((len(wanted),)),
            pltpu.SemaphoreType.DMA((2, CHUNKS)),
        ],
        compiler_params=pltpu.CompilerParams(vmem_limit_bytes=FIRST_LIMIT << 20),
        cost_estimate=pl.CostEstimate(
            flops=2 * used * BLOCK * half * depth,
            bytes_accessed=4 * depth * (rows + width),
            transcendentals=0,
        ),
    )(activations, out_grads)


def added(outs, steps=1):
    operands, in_specs = [], []
    width = outs[0][1][0][0].shape[1]
    piece = width // steps
    for _, terms in outs:
        for value, start, size, _ in terms:
            operands.append(value)
            in_specs.append(
                pl.BlockSpec((size, piece), functools.partial(lambda s, i: (s, i), start // size))
            )

    def body(*refs):
        at = 0
        for (rows, terms), out in zip(outs, refs[len(operands) :]):
            edges = sorted({0, rows} | {t[3] for t in terms} | {t[3] + t[2] for t in terms})
            for low, high in zip(edges, edges[1:]):
                total = None
                for k, (_, _, size, place) in enumerate(terms):
                    if place <= low and high <= place + size:
                        value = refs[at + k][low - place : high - place, :].astype(f32)
                        total = value if total is None else total + value
                out[low:high, :] = total.astype(bf16)
            at += len(terms)

    return pl.pallas_call(
        body,
        grid=(steps,),
        in_specs=in_specs,
        out_specs=[pl.BlockSpec((rows, piece), lambda i: (0, i)) for rows, _ in outs],
        out_shape=[jax.ShapeDtypeStruct((rows, width), bf16) for rows, _ in outs],
        compiler_params=pltpu.CompilerParams(vmem_limit_bytes=24 << 20),
        cost_estimate=pl.CostEstimate(flops=1 << 20, bytes_accessed=1 << 20, transcendentals=0),
    )(*operands)


def kernel(body, operands, in_specs, out_specs, out_shape, aliases, steps=1):
    return pl.pallas_call(
        body,
        grid=(steps,),
        in_specs=in_specs,
        out_specs=out_specs,
        out_shape=out_shape,
        input_output_aliases=aliases,
        compiler_params=pltpu.CompilerParams(vmem_limit_bytes=16 << 20),
        cost_estimate=pl.CostEstimate(flops=2 << 20, bytes_accessed=3 << 20, transcendentals=0),
    )(*operands)


SMEM = pl.BlockSpec(memory_space=pltpu.SMEM)


def compress(side, factor, params, estimate, exponents, terms):
    rows, width = params.shape[1:]
    half = width // 2
    span = rows // exponents.shape[1]
    big = pl.BlockSpec((1, rows, half), lambda i: (0, 0, side))
    flat = pl.BlockSpec((rows, half), lambda i: (0, 0))
    operands = [exponents, params, estimate]
    in_specs = [SMEM, big, big]
    for value, start in terms:
        operands.append(value)
        in_specs.append(pl.BlockSpec((rows, half), lambda i, s=start // rows: (s, 0)))

    def body(*refs):
        e_ref, p_ref, s_ref = refs[:3]
        comp_ref, stepped_ref = refs[len(operands) :]
        for part in range(rows // span):
            exponent = e_ref[0, part]
            scale = jnp.left_shift(jnp.int32(1), exponent).astype(f32)
            inverse = jnp.left_shift(jnp.int32(1), 24 - exponent).astype(f32) * (2.0**-24)
            cut = slice(part * span, (part + 1) * span)
            gradient = refs[3][cut, :].astype(f32)
            for k in range(1, len(terms)):
                gradient = gradient + refs[3 + k][cut, :].astype(f32)
            stepped = p_ref[0, cut, :] - factor * gradient
            change = stepped - s_ref[0, cut, :]
            levels = jnp.clip(change * inverse, -1.0, 1.0).astype(bf16)
            comp_ref[cut, :] = (levels.astype(f32) * scale).astype(bf16)
            stepped_ref[cut, :] = stepped

    shapes = [jax.ShapeDtypeStruct((rows, half), bf16), jax.ShapeDtypeStruct((rows, half), f32)]
    return kernel(body, operands, in_specs, [flat, flat], shapes, {})


def own_part(side, estimate, mixed_sum, edge_weight, compressed, stepped, held, after):
    rows, width = estimate.shape[1:]
    half = width // 2
    big = pl.BlockSpec((1, rows, half), lambda i: (0, 0, side))
    flat = pl.BlockSpec((rows, half), lambda i: (0, 0))
    operands = [edge_weight, estimate, mixed_sum, compressed, stepped]
    in_specs = [SMEM, big, big, flat, flat]
    aliases = {}
    if held is not None:
        aliases = {len(operands): 2}
        operands.append(held)
        in_specs.append(ANY)
    operands += after
    in_specs += [ANY] * len(after)

    def body(*refs):
        w_ref, s_ref, m_ref, c_ref, p_ref = refs[:5]
        base_ref, rest_ref, est_ref = refs[len(operands) :]
        group = lax.axis_index("grp")
        right, left = w_ref[group], w_ref[lax.rem(group + 7, 8)]
        own = c_ref[...].astype(f32)
        new = s_ref[0] + own
        base_ref[...] = m_ref[0] + (1.0 - left - right) * own
        rest_ref[...] = p_ref[...] - mixing_rate * new
        est_ref[0] = new

    shapes = [jax.ShapeDtypeStruct((rows, half), f32)] * 2
    shapes.append(jax.ShapeDtypeStruct(estimate.shape, f32))
    return kernel(body, operands, in_specs, [flat, flat, big], shapes, aliases)


def finish(side, edge_weight, base, rest, from_far, from_near, held, shape):
    rows, width = shape[1:]
    half = width // 2
    piece = half // 2
    big = pl.BlockSpec((1, rows, piece), lambda i: (0, 0, side * 2 + i))
    flat = pl.BlockSpec((rows, piece), lambda i: (0, i))
    operands = [edge_weight, base, rest, from_far, from_near]
    in_specs = [SMEM, flat, flat, flat, flat]
    aliases = {}
    if held is not None:
        aliases = {len(operands): 0, len(operands) + 1: 1}
        operands += list(held)
        in_specs += [ANY, ANY]

    def body(*refs):
        w_ref, base_ref, rest_ref, far_ref, near_ref = refs[:5]
        new_params, new_mixed = refs[len(operands) :]
        group = lax.axis_index("grp")
        right, left = w_ref[group], w_ref[lax.rem(group + 7, 8)]
        odd = lax.rem(group, 2) == 1
        mixed = base_ref[...] + jnp.where(odd, right, left) * far_ref[...].astype(f32)
        mixed = mixed + jnp.where(odd, left, right) * near_ref[...].astype(f32)
        new_mixed[0] = mixed
        new_params[0] = rest_ref[...] + mixing_rate * mixed

    shapes = [jax.ShapeDtypeStruct(shape, f32)] * 2
    return kernel(body, operands, in_specs, [big, big], shapes, aliases, 2)


def on_device(params, estimate, mixed_sum, activations, out_grads, exponents, edge_weight):
    factor = step_size / math.sqrt(lax.axis_size("mem") * activations.shape[0])
    low = BLOCK // 2
    theirs_1, mine_1, activations, out_grads = first_products(
        activations, out_grads, 1, SENT_B, [place for task in KEPT_B for place in task]
    )
    other_1 = to_partner(theirs_1)
    theirs_2, mine_2 = products(activations, out_grads, 0, SENT_A, [theirs_1])
    other_2 = to_partner(theirs_2)

    def pair(mine, other, start, size, *more):
        return (size, [(mine, start, size, 0), (other, start, size, 0), *more])

    pair_1 = functools.partial(pair, mine_1, other_1)
    pair_2 = functools.partial(pair, mine_2, other_2)
    a_up, a_down = added([pair_2(0, 256), pair_2(256, 256)])
    got_up, got_down = up(a_up), down(a_down)
    b_above, b_below, b_far, b_own = added([pair_1(k * BLOCK, BLOCK) for k in range(4)])
    got_far = to_side(b_far)
    got_above, got_below = to_side(b_above), to_side(b_below)
    got_own = to_side(b_own)
    theirs_3, mine_3 = products(activations, out_grads, 1, KEPT_B, [a_up, b_far])
    other_3 = to_partner(theirs_3)
    theirs_4, mine_4 = products(activations, out_grads, 0, KEPT_A, [theirs_3])
    other_4 = to_partner(theirs_4)
    pair_3 = functools.partial(pair, mine_3, other_3)
    pair_4 = functools.partial(pair, mine_4, other_4)
    far_low, far_high = added(
        [
            pair_3(0, low, (got_far, 0, low, 0)),
            pair_3(low, low, (got_far, low, low, 0)),
        ],
    )
    far_low, far_high = up(far_low), down(far_high)
    send_down = added([pair_4(BLOCK, BLOCK, (got_down, 0, BLOCK, 0))])[0]
    send_up = added([pair_4(0, BLOCK, (got_up, 0, BLOCK, 0))])[0]
    from_below, from_above = up(send_up), down(send_down)
    v_up = added([pair_3(256, BLOCK, (got_above, 0, BLOCK, 0), (far_low, 0, low, 0))])[0]
    v_down = added([pair_3(384, BLOCK, (got_below, 0, BLOCK, 0), (far_high, 0, low, low))])[0]
    b_below, b_above = up(v_up), down(v_down)
    side_sum = added([pair_4(384, BLOCK, (got_up, BLOCK, BLOCK, 0), (from_above, 0, BLOCK, 0))])[0]
    got_side = to_side(side_sum)
    terms_b = [(mine_3, BLOCK), (other_3, BLOCK), (got_own, 0), (b_below, 0), (b_above, 0)]
    terms_a = [(mine_4, 256), (other_4, 256), (got_down, BLOCK), (from_below, 0), (got_side, 0)]
    comp_b, stepped_b = compress(1, factor, params, estimate, exponents, terms_b)
    far_b, near_b = far_pairs(comp_b), near_pairs(comp_b)
    comp_a, stepped_a = compress(0, factor, params, estimate, exponents, terms_a)
    far_a, near_a = far_pairs(comp_a), near_pairs(comp_a)
    own = (estimate, mixed_sum, edge_weight)
    base_b, rest_b, held = own_part(1, *own, comp_b, stepped_b, None, [comp_a])
    base_a, rest_a, new_estimate = own_part(0, *own, comp_a, stepped_a, held, [])
    outs = finish(1, edge_weight, base_b, rest_b, far_b, near_b, None, params.shape)
    new_params, new_mixed = finish(
        0, edge_weight, base_a, rest_a, far_a, near_a, outs, params.shape
    )
    return (new_params, new_estimate, new_mixed)


def solution(mesh):
    in_specs = (
        P("grp", "mem", None),
        P("grp", "mem", None),
        P("grp", "mem", None),
        P(("grp", "mem"), None),
        P(("grp", "mem"), None),
        P("grp", "mem"),
        P(),
    )
    out_specs = (P("grp", "mem", None), P("grp", "mem", None), P("grp", "mem", None))
    return jax.shard_map(
        on_device, mesh=mesh, in_specs=in_specs, out_specs=out_specs, check_vma=False
    )
```
